32 devices in a mesh: lat: 16 (over z, y, x), ord: 2 (over core).
Axes of the slice: x: 2, y: 2, z: 4, core: 2. Of those that a mesh axis runs over, the one named last changes fastest.
Arguments:
- pressure: bfloat16 [2, 128, 5760], P(None, 'lat', 'ord'), may hold values from -6 to 6
- tables: bfloat16 [512, 128, 2048], P('ord', 'lat'), may hold values from -6 to 6
- quad_weight: float32 [128], replicated, may hold values from 0.5 to 2
- love_number: float32 [2048], replicated, may hold values from -0.5 to 0
- order_list: int32 [512], replicated, may hold values from 0 to 511, each once
- cycle_list: int32 [128], P('lat'), may hold values from 0 to 127, each once
Outputs:
- spectrum: float32 [2, 512, 2048], P(None, 'ord', 'lat')
- load_field: float32 [2, 128, 5760], P(None, 'lat', 'ord')
The draws below stay inside these ranges and needn't reach their ends.
Inputs may be any that keep to these rules, and one draw needn't show every extreme that they name: `order_list`: every order from 0 to 511 stands in exactly one slot. `cycle_list`: every northern cycle from 0 to 127 stands in exactly one slot; the same slot of the southern half holds its mirror cycle.
All inputs are finite; a program needn't handle non-finite values.
Results may differ from the reference program's by a relative error of at most 0.0055.
Values may be sent and summed in bfloat16 or wider, within the bound.
A program may use at most 64 MiB of HBM per device.

```python
import math
import jax
import jax.numpy as jnp
from jax import lax

NLON = 5760
LDEG = 2048
NORD = 512
NHALF = 128


def with_spikes(array, stream_key, source, target, blocks, factor):
    def block_of(dim):
        return (jnp.arange(array.shape[dim]) // (array.shape[dim] // blocks)).reshape((-1,) + (1,) * (array.ndim - 1 - dim))

    near = jax.random.permutation(stream_key, blocks)[block_of(target)]
    other_side = (block_of(target) + blocks // 2) % blocks
    return jnp.where((block_of(source) == near) | (block_of(source) == other_side), factor * array, array)


def levels(stream_key, extent, pieces, smallest, high):
    level, own = 1.0, jax.random.fold_in(stream_key, 6)
    for dim, blocks in pieces:
        draws = jnp.exp(jax.random.uniform(jax.random.fold_in(own, dim), (blocks,), jnp.float32, smallest / len(pieces), high / len(pieces)))
        level = level * jnp.repeat(draws, extent[dim] // blocks).reshape([-1 if axis == dim else 1 for axis in range(len(extent))])
    return level


def normal_values(own_key, dims, scale, limit, cuts=(), kind=jnp.bfloat16):
    result = jax.random.normal(own_key, dims, jnp.float32) * scale
    if len(cuts) > 0:
        result = levels(own_key, dims, cuts, -0.22, 0.18) * result
    return jnp.clip(result, min=-limit, max=limit).astype(kind)


def heavy_noise(own_key, extent, scale, reach, pieces, heavy, held_as=jnp.bfloat16):
    values = scale * jax.random.normal(own_key, extent, jnp.float32)
    if pieces:
        values = values * levels(own_key, extent, pieces, -0.22, 0.18)
    return jnp.clip(with_spikes(values, jax.random.fold_in(own_key, 3), *heavy), -reach, reach).astype(held_as)


def setup_inputs(seed: int = 0) -> dict:
    splits = jax.random.split(jax.random.key(seed), 7)
    return {
        "pressure": normal_values(splits[0], (2, NHALF, NLON), 1.0, 6.0, ((1, 16), (2, 2))),
        "tables": heavy_noise(splits[1], (NORD, NHALF, LDEG), 1.0, 6.0, ((0, 2), (1, 16)), (1, 2, 16, 2.0)),
        "quad_weight": jnp.clip(jnp.exp(jax.random.uniform(splits[2], (NHALF,), jnp.float32, math.log(0.5), math.log(2.0))), 0.5, 2.0),
        "love_number": jnp.clip(jax.random.uniform(splits[3], (LDEG,), jnp.float32, -0.5, 0.0), -0.5, 0.0),
        "order_list": jax.random.permutation(splits[4], NORD).astype(jnp.int32),
        "cycle_list": jax.random.permutation(splits[5], NHALF).astype(jnp.int32),
    }


DENSITY_RATIO = 3.0 * 1025.0 / 5517.0

def phase_table(order_values, positions):
    phase = order_values[:, None] * positions[None, :] % NLON
    angle = phase.astype(jnp.float32) * (2.0 * math.pi / NLON)
    return (jnp.cos(angle).astype(jnp.bfloat16), jnp.sin(angle).astype(jnp.bfloat16))

def reference(pressure, tables, quad_weight, love_number, order_list, cycle_list):
    grid_rows = pressure.reshape(2 * NHALF, NLON)
    cosine_table, sine_table = phase_table(order_list, jnp.arange(NLON, dtype=jnp.int32))
    lon_scale = 1.0 / math.sqrt(NLON)
    real_part = lon_scale * jnp.dot(grid_rows, cosine_table.T, preferred_element_type=jnp.float32)
    imag_part = -lon_scale * jnp.dot(grid_rows, sine_table.T, preferred_element_type=jnp.float32)
    cycle_weight = (quad_weight[cycle_list] * (1.0 / math.sqrt(NHALF)))[:, None]
    north_real = real_part[:NHALF]
    south_real = real_part[NHALF:]
    north_imag = imag_part[:NHALF]
    south_imag = imag_part[NHALF:]
    folded = jnp.stack([cycle_weight * (north_real + south_real), cycle_weight * (north_imag + south_imag), cycle_weight * (north_real - south_real), cycle_weight * (north_imag - south_imag)], 0)
    folded = jnp.transpose(folded.astype(jnp.bfloat16), (2, 1, 0))
    degree = jnp.arange(LDEG, dtype=jnp.int32)

    def analyse(item):
        table, column, order_value = item
        product = jnp.dot(column.T, table, preferred_element_type=jnp.float32)
        even = (degree + order_value) % 2 == 0
        present = degree >= order_value
        coeff_real = jnp.where(present, jnp.where(even, product[0], product[2]), 0.0)
        coeff_imag = jnp.where(present, jnp.where(even, product[1], product[3]), 0.0)
        return jnp.stack([coeff_real, coeff_imag], 0)
    coefficients = lax.map(analyse, (tables, folded, order_list))
    spectrum = jnp.transpose(coefficients, (1, 0, 2))
    love_factor = DENSITY_RATIO * (1.0 + love_number)
    scaled = (love_factor * coefficients).astype(jnp.bfloat16)
    deg_scale = 1.0 / math.sqrt(LDEG)

    def synthesise(item):
        table, coeff, order_value = item
        even = (degree + order_value) % 2 == 0
        zero = jnp.zeros_like(coeff[0])
        stacked = jnp.stack([jnp.where(even, coeff[0], zero), jnp.where(even, coeff[1], zero), jnp.where(even, zero, coeff[0]), jnp.where(even, zero, coeff[1])], 0)
        summed = jnp.dot(table, stacked.T, preferred_element_type=jnp.float32)
        north = deg_scale * (summed[:, :2] + summed[:, 2:])
        south = deg_scale * (summed[:, :2] - summed[:, 2:])
        return jnp.stack([north, south], 0).astype(jnp.bfloat16)
    synthesised = lax.map(synthesise, (tables, scaled, order_list))
    synth_real = synthesised[..., 0].reshape(NORD, 2 * NHALF)
    synth_imag = synthesised[..., 1].reshape(NORD, 2 * NHALF)
    field = jnp.dot(synth_real.T, cosine_table, preferred_element_type=jnp.float32) - jnp.dot(synth_imag.T, sine_table, preferred_element_type=jnp.float32)
    load_field = (1.0 / math.sqrt(NORD) * field).reshape(2, NHALF, NLON)
    return (spectrum, load_field)
```

```python
import functools
import math

import jax
import jax.numpy as jnp
import numpy as np
from jax import lax
from jax.experimental import pallas as pl
from jax.experimental.pallas import tpu as pltpu
from jax.sharding import PartitionSpec as P

DENSITY_RATIO = 3.0 * 1025.0 / 5517.0
LANES = 128
GROUPS = 8
STAGGER = 4
MESH = pl.DeviceIdType.MESH
NT = (((1,), (1,)), ((), ()))
F32 = jnp.float32
BF16 = jnp.bfloat16


def bit_orders(bits):
    base = list(range(bits))
    if bits < 3:
        return [base] * GROUPS
    a = base
    b = [1, 0] + base[2:]
    c = [2, 0, 1] + base[3:]
    d = [2, 1, 0] + base[3:]
    e = [0, 2, 1] + base[3:]
    f = [1, 2, 0] + base[3:]
    return [a, b, c, e, f, d, a, b]


def permuted(index, order):
    bits = len(order)
    return sum(((index // 2**b) % 2) * 2 ** (bits - 1 - at) for at, b in enumerate(order))


def twiddles(no, lon_local, orders):
    blocks = -(-lon_local // LANES)
    period = no * lon_local

    def turn(positions):
        phase = np.outer(positions, np.arange(orders)) % period
        angle = phase * (2.0 * math.pi / period)
        return np.cos(angle), np.sin(angle)

    fine = np.concatenate(turn(np.arange(LANES)), 1)
    high = fine.astype(BF16)
    low = (fine - high.astype(np.float64)).astype(BF16)
    starts = (lon_local * np.arange(no)[:, None] + LANES * np.arange(blocks)).reshape(-1)
    cos, sin = turn(starts)
    return np.concatenate([high, low], 0), cos.astype(np.float32), sin.astype(np.float32)


def kernel(
    n, no,
    press_hbm, tables_ref, quad_hbm, love_hbm, order_hbm, cycle_hbm, fine_hbm, cos_hbm, sin_hbm,
    spec_ref, field_ref,
    tab, press_ref, quad_ref, love_ref, order_ref, cycle_ref, fine, cos_q, sin_q,
    gathered, wide, partial, orders_ref, pick, lhs, part, landed, scaled,
    natural, rotated, out_signal, in_signal,
    tab_sem, in_sem, press_sem, rs_sem, ag_sem, field_sem,
):
    bits = n.bit_length() - 1
    me = lax.axis_index("lat")
    core = lax.axis_index("ord")
    cycles = press_ref.shape[1]
    lon_local = press_ref.shape[2]
    local_orders = orders_ref.shape[0]
    degrees = tables_ref.shape[1]
    share = degrees // n
    go = local_orders // GROUPS
    rows_g = go * cycles
    both = 2 * cycles
    blocks = max(1, min(n, 1024 // share))
    width = blocks * share
    orders_of = bit_orders(bits)
    period = lon_local * no
    turns = cos_q.shape[0] // no
    modes = order_ref.shape[1]

    barrier = pltpu.get_barrier_semaphore()
    partners = []
    for b in range(bits):
        mine = (me // 2**b) % 2
        partners.append(me + (1 - 2 * mine) * 2**b)
    peers = [lax.rem(core + i, no) for i in range(1, no)]
    for peer in peers:
        pl.semaphore_signal(barrier, inc=1, device_id=(me, peer), device_id_type=MESH)
    for partner in partners:
        pl.semaphore_signal(barrier, inc=1, device_id=(partner, core), device_id_type=MESH)

    loads = []
    pairs = (
        (press_hbm, press_ref), (order_hbm, order_ref), (quad_hbm, quad_ref), (cycle_hbm, cycle_ref),
        (fine_hbm, fine), (cos_hbm, cos_q), (sin_hbm, sin_q), (love_hbm, love_ref),
    )
    for i, (source, to) in enumerate(pairs):
        copy = pltpu.make_async_copy(source, to, in_sem.at[i])
        copy.start()
        loads.append(copy)
    tab_copies = []
    for g in range(GROUPS):
        rows = pl.ds(g * rows_g, rows_g)
        copy = pltpu.make_async_copy(tables_ref.at[rows], tab.at[rows], tab_sem.at[g])
        copy.start()
        tab_copies.append(copy)

    pl.semaphore_wait(barrier, bits + no - 1)
    loads[0].wait()
    press_copies = []
    for i, peer in enumerate(peers):
        copy = pltpu.make_async_remote_copy(
            src_ref=press_ref,
            dst_ref=gathered.at[i],
            send_sem=press_sem.at[0, i],
            recv_sem=press_sem.at[1, i],
            device_id=(me, peer),
            device_id_type=MESH,
        )
        copy.start()
        press_copies.append(copy)

    def widen(at, piece):
        for q in range(turns):
            first = q * LANES
            count = min(LANES, lon_local - first)
            rows = jnp.concatenate([piece[h, :, first : first + count].astype(F32) for h in range(2)], 0)
            if count < LANES:
                rows = jnp.concatenate([rows, jnp.zeros((both, LANES - count), F32)], 1)
            rows = rows.astype(BF16)
            wide[at, q * both : (q + 1) * both, :LANES] = rows
            wide[at, q * both : (q + 1) * both, LANES:] = rows

    def transform(at, origin, start):
        partial[...] = jnp.dot(wide[at], fine[...], preferred_element_type=F32)

        def turn(q, carry):
            cos_sum, sin_sum = carry
            rows = pl.ds(pl.multiple_of(q * both, both), both)
            c = partial[rows, :modes]
            s = partial[rows, modes:]
            cq = cos_q[pl.ds(origin * turns + q, 1), :]
            sq = sin_q[pl.ds(origin * turns + q, 1), :]
            return cos_sum + (cq * c - sq * s), sin_sum + (sq * c + cq * s)

        return lax.fori_loop(0, turns, turn, start)

    widen(0, press_ref)
    for copy in loads[1:]:
        copy.wait()
    shape = (local_orders, modes)
    slot = core * local_orders + lax.broadcasted_iota(jnp.int32, shape, 0)
    lane = lax.broadcasted_iota(jnp.int32, shape, 1)
    order_col = jnp.sum(
        jnp.where(slot == lane, order_ref[...].astype(F32), 0.0), axis=1, keepdims=True
    ).astype(jnp.int32)
    orders_ref[...] = order_col
    pick[...] = jnp.where(order_col == lane, 1.0, 0.0).astype(BF16)

    square = (cycles, cycles)
    eye = lax.broadcasted_iota(jnp.int32, square, 0) == lax.broadcasted_iota(jnp.int32, square, 1)
    cycle_col = jnp.sum(
        jnp.where(eye, cycle_ref[...].astype(F32), 0.0), axis=1, keepdims=True
    ).astype(jnp.int32)
    quad_lane = lax.broadcasted_iota(jnp.int32, (cycles, quad_ref.shape[1]), 1)
    weight = jnp.sum(jnp.where(quad_lane == cycle_col, quad_ref[...], 0.0), axis=1, keepdims=True)
    weight = weight * (1.0 / math.sqrt(quad_ref.shape[1])) * (1.0 / math.sqrt(period))

    col = lax.broadcasted_iota(jnp.int32, (go, rows_g), 1) // cycles
    row = lax.broadcasted_iota(jnp.int32, (go, rows_g), 0)
    diagonal = row == col
    spread_row = lax.broadcasted_iota(jnp.int32, (4 * cycles, 4 * rows_g), 0)
    spread_col = lax.broadcasted_iota(jnp.int32, (4 * cycles, 4 * rows_g), 1)
    spread = jnp.where(
        spread_row == (spread_col // rows_g) * cycles + spread_col % cycles, 1.0, 0.0
    ).astype(BF16)
    pick_row = lax.broadcasted_iota(jnp.int32, (cycles, rows_g), 0)
    pick_col = lax.broadcasted_iota(jnp.int32, (cycles, rows_g), 1)
    gather_rows = jnp.where(pick_row == pick_col % cycles, 1.0, 0.0).astype(BF16)

    zero = jnp.zeros((both, modes), F32)
    sums = transform(0, core, (zero, zero))
    for i, copy in enumerate(press_copies):
        copy.wait()
        widen(i + 1, gathered.at[i])
        sums = transform(i + 1, lax.rem(core + no - 1 - i, no), sums)
    cos_sum, sin_sum = sums
    folded = jnp.concatenate(
        [
            weight * (cos_sum[:cycles] + cos_sum[cycles:]),
            -weight * (sin_sum[:cycles] + sin_sum[cycles:]),
            weight * (cos_sum[:cycles] - cos_sum[cycles:]),
            -weight * (sin_sum[:cycles] - sin_sum[cycles:]),
        ],
        0,
    ).astype(BF16)
    chosen = lax.dot_general(pick[...], folded, NT, preferred_element_type=F32).astype(BF16)
    repeated = jnp.dot(chosen, spread, preferred_element_type=F32)
    for g in range(GROUPS):
        rows = repeated[g * go : (g + 1) * go]
        lhs[g] = jnp.concatenate(
            [jnp.where(diagonal, rows[:, c * rows_g : (c + 1) * rows_g], 0.0) for c in range(4)], 0
        ).astype(BF16)

    def parity(g, first):
        degree = first + lax.broadcasted_iota(jnp.int32, (go, width), 1)
        order = orders_ref[g * go : (g + 1) * go, :]
        return (degree + order) & 1 == 0, degree >= order

    def region(g, k):
        base = 0
        for at in range(k):
            base = base + ((me // 2 ** orders_of[g][at]) % 2) * (n >> (at + 1))
        return base

    def analyse(g):
        tab_copies[g].wait()
        left = lhs[g]
        for i in range(degrees // width):
            first = i * width
            product = jnp.dot(
                left, tab[g * rows_g : (g + 1) * rows_g, pl.ds(first, width)], preferred_element_type=F32
            )
            even, present = parity(g, first)
            real = jnp.where(present, jnp.where(even, product[:go], product[2 * go : 3 * go]), 0.0)
            imag = jnp.where(present, jnp.where(even, product[go : 2 * go], product[3 * go :]), 0.0)
            value = jnp.concatenate([real, imag], 0).astype(BF16)
            for j in range(blocks):
                to = permuted(i * blocks + j, orders_of[g])
                part[g, to] = value[:, j * share : (j + 1) * share]

    reduce_copies = {}
    gather_copies = {}

    def send_reduce(g, k):
        h = n >> (k + 1)
        b = orders_of[g][k]
        mine = (me // 2**b) % 2
        copy = pltpu.make_async_remote_copy(
            src_ref=part.at[g, pl.ds(region(g, k) + (1 - mine) * h, h)],
            dst_ref=landed.at[g, pl.ds(n - (n >> k), h)],
            send_sem=rs_sem.at[0, g, k],
            recv_sem=rs_sem.at[1, g, k],
            device_id=(partners[b], core),
            device_id_type=MESH,
        )
        copy.start()
        reduce_copies[g, k] = copy

    def take_reduce(g, k):
        h = n >> (k + 1)
        reduce_copies[g, k].wait_recv()
        keep = region(g, k + 1)
        off = n - (n >> k)
        if k < bits - 1:

            def add(i, carry):
                part[g, keep + i] = (
                    part[g, keep + i].astype(F32) + landed[g, off + i].astype(F32)
                ).astype(BF16)
                return carry

            lax.fori_loop(0, h, add, 0, unroll=min(h, 4))
            send_reduce(g, k + 1)
            return
        total = part[g, keep].astype(F32) + landed[g, off].astype(F32)
        spec_ref[0, g * go : (g + 1) * go, :] = total[:go]
        spec_ref[1, g * go : (g + 1) * go, :] = total[go:]
        scaled[g, keep] = (DENSITY_RATIO * (1.0 + love_ref[pl.ds(me, 1), :]) * total).astype(BF16)
        send_gather(g, bits - 1)

    def send_gather(g, k):
        h = n >> (k + 1)
        b = orders_of[g][k]
        mine = pl.ds(region(g, k + 1), h)
        copy = pltpu.make_async_remote_copy(
            src_ref=scaled.at[g, mine],
            dst_ref=scaled.at[g, mine],
            send_sem=ag_sem.at[0, g, k],
            recv_sem=ag_sem.at[1, g, k],
            device_id=(partners[b], core),
            device_id_type=MESH,
        )
        copy.start()
        gather_copies[g, k] = copy

    def take_gather(g, k):
        gather_copies[g, k].wait_recv()
        if k > 0:
            send_gather(g, k - 1)

    def synthesise(g):
        def chunk(i, total):
            first = pl.multiple_of(i * width, width)
            even, _ = parity(g, first)
            pieces = [scaled[g, permuted(i * blocks + j, orders_of[g])] for j in range(blocks)]
            both = jnp.concatenate(pieces, 1).astype(F32)
            real, imag = both[:go], both[go:]
            stacked = jnp.concatenate(
                [real, imag, jnp.where(even, real, -real), jnp.where(even, imag, -imag)], 0
            ).astype(BF16)
            return total + lax.dot_general(
                stacked, tab[g * rows_g : (g + 1) * rows_g, pl.ds(first, width)], NT,
                preferred_element_type=F32,
            )

        total = lax.fori_loop(0, degrees // width, chunk, jnp.zeros((4 * go, rows_g), F32))
        total = total * (1.0 / math.sqrt(degrees))
        signal = jnp.concatenate(
            [
                lax.dot_general(
                    gather_rows,
                    jnp.where(diagonal, total[c * go : (c + 1) * go], 0.0).astype(BF16),
                    NT, preferred_element_type=F32,
                )
                for c in range(4)
            ],
            0,
        )
        piece = jnp.dot(
            signal.astype(BF16), pick[g * go : (g + 1) * go, :], preferred_element_type=F32
        )
        natural[...] = piece if g == 0 else natural[...] + piece

    steps = []
    for g in range(GROUPS):
        steps.append((g, g, lambda g=g: (analyse(g), send_reduce(g, 0))))
        for k in range(bits):
            steps.append((g + STAGGER * (k + 1), g, lambda g=g, k=k: take_reduce(g, k)))
        for i, k in enumerate(reversed(range(bits))):
            steps.append((g + STAGGER * (bits + i + 1), g, lambda g=g, k=k: take_gather(g, k)))
        steps.append((g + STAGGER * 2 * bits + 0.5, g, lambda g=g: synthesise(g)))
    for _, _, step in sorted(steps, key=lambda s: (s[0], s[1])):
        step()

    out_signal[...] = natural[...].astype(BF16)
    field_copies = []
    for i, peer in enumerate(peers):
        copy = pltpu.make_async_remote_copy(
            src_ref=out_signal,
            dst_ref=in_signal.at[i],
            send_sem=field_sem.at[0, i],
            recv_sem=field_sem.at[1, i],
            device_id=(me, peer),
            device_id_type=MESH,
        )
        copy.start()
        field_copies.append(copy)
    total = out_signal[...].astype(F32)
    for i, copy in enumerate(field_copies):
        copy.wait_recv()
        total = total + in_signal[i].astype(F32)
    total = total * (1.0 / math.sqrt(modes))
    real = jnp.concatenate([total[:cycles], total[2 * cycles : 3 * cycles]], 0)
    imag = jnp.concatenate([total[cycles : 2 * cycles], total[3 * cycles :]], 0)
    for q in range(turns):
        cq = cos_q[pl.ds(core * turns + q, 1), :]
        sq = sin_q[pl.ds(core * turns + q, 1), :]
        rows = slice(q * both, (q + 1) * both)
        rotated[rows, :modes] = (real * cq - imag * sq).astype(BF16)
        rotated[rows, modes:] = (-real * sq - imag * cq).astype(BF16)
    parts = lax.dot_general(rotated[...], fine[...], NT, preferred_element_type=F32)
    field = parts[:, :LANES] + parts[:, LANES:]
    for q in range(turns):
        first = q * LANES
        count = min(LANES, lon_local - first)
        for h in range(2):
            at = q * both + h * cycles
            field_ref[h, :, first : first + count] = field[at : at + cycles, :count]
    for copy in list(reduce_copies.values()) + list(gather_copies.values()) + field_copies:
        copy.wait_send()


def finish(half_spec, half_field, spec_ref, field_ref):
    spec_ref[...] = half_spec[...]
    field_ref[...] = half_field[...]


def per_device(n, no, pressure, tables, quad_weight, love_number, order_list, cycle_list):
    _, cycles, lon_local = pressure.shape
    local_orders, _, degrees = tables.shape
    bits = n.bit_length() - 1
    share = degrees // n
    go = local_orders // GROUPS
    rows_g = go * cycles
    modes = order_list.shape[0]
    turns = -(-lon_local // LANES)
    fine, cos_q, sin_q = [jnp.asarray(table) for table in twiddles(no, lon_local, modes)]
    small = (
        quad_weight[None, :], love_number.reshape(n, share), order_list[None, :], cycle_list[None, :],
        fine, cos_q, sin_q,
    )
    vmem = pl.BlockSpec(memory_space=pltpu.VMEM)
    hbm = pl.BlockSpec(memory_space=pl.ANY)
    blocks = pltpu.VMEM((GROUPS, n, 2 * go, share), BF16)
    spectrum, field = pl.pallas_call(
        functools.partial(kernel, n, no),
        out_shape=(
            jax.ShapeDtypeStruct((2, local_orders, share), F32),
            jax.ShapeDtypeStruct((2, cycles, lon_local), F32),
        ),
        in_specs=[hbm] * 9,
        out_specs=(vmem, vmem),
        scratch_shapes=[
            pltpu.VMEM((local_orders * cycles, degrees), BF16),
            pltpu.VMEM((2, cycles, lon_local), BF16),
            *[pltpu.VMEM(array.shape, array.dtype) for array in small],
            pltpu.VMEM((no - 1, 2, cycles, lon_local), BF16),
            pltpu.VMEM((no, turns * 2 * cycles, 2 * LANES), BF16),
            pltpu.VMEM((turns * 2 * cycles, 2 * modes), F32),
            pltpu.VMEM((local_orders, 1), jnp.int32),
            pltpu.VMEM((local_orders, modes), BF16),
            pltpu.VMEM((GROUPS, 4 * go, rows_g), BF16),
            blocks, blocks, blocks,
            pltpu.VMEM((4 * cycles, modes), F32),
            pltpu.VMEM((turns * 2 * cycles, 2 * modes), BF16),
            pltpu.VMEM((4 * cycles, modes), BF16),
            pltpu.VMEM((no - 1, 4 * cycles, modes), BF16),
            pltpu.SemaphoreType.DMA((GROUPS,)),
            pltpu.SemaphoreType.DMA((8,)),
            pltpu.SemaphoreType.DMA((2, no - 1)),
            pltpu.SemaphoreType.DMA((2, GROUPS, bits)),
            pltpu.SemaphoreType.DMA((2, GROUPS, bits)),
            pltpu.SemaphoreType.DMA((2, no - 1)),
        ],
        compiler_params=pltpu.CompilerParams(
            collective_id=0, has_side_effects=True, vmem_limit_bytes=56 * 1024 * 1024
        ),
    )(pressure, tables.reshape(local_orders * cycles, degrees), *small)
    return pl.pallas_call(
        finish,
        out_shape=(
            jax.ShapeDtypeStruct(spectrum.shape, F32),
            jax.ShapeDtypeStruct(field.shape, F32),
        ),
        in_specs=[vmem, vmem],
        out_specs=(vmem, vmem),
    )(spectrum, field)


def solution(mesh):
    placed = (P(None, "lat", "ord"), P("ord", "lat", None), P(), P(), P(), P("lat"))
    return jax.shard_map(
        functools.partial(per_device, mesh.shape["lat"], mesh.shape["ord"]),
        mesh=mesh,
        in_specs=placed,
        out_specs=(P(None, "ord", "lat"), P(None, "lat", "ord")),
        check_vma=False,
    )
```

```python
import functools
import math

import jax
import jax.numpy as jnp
import numpy as np
from jax import lax
from jax.experimental import pallas as pl
from jax.experimental.pallas import tpu as pltpu
from jax.sharding import PartitionSpec as P

DENSITY_RATIO = 3.0 * 1025.0 / 5517.0
LANES = 128
UNITS = 8
STAGGER = 4
MESH = pl.DeviceIdType.MESH
NT = (((1,), (1,)), ((), ()))
F32 = jnp.float32
BF16 = jnp.bfloat16


PLAN_ORDERS = (
    (1, 3, 0, 2), (2, 0, 1, 3), (1, 2, 0, 3), (0, 1, 2, 3), (1, 0, 3, 2), (0, 2, 1, 3),
    (1, 0, 3, 2), (2, 1, 3, 0), (0, 2, 1, 3), (0, 2, 1, 3), (2, 0, 1, 3), (2, 3, 0, 1),
    (2, 0, 1, 3), (1, 0, 2, 3), (0, 1, 2, 3), (1, 0, 3, 2),
)
PLAN_STEPS = (
    192, 224, 96, 160, 128, 209, 193, 0, 32, 97, 241, 64, 210, 129, 1, 177, 145, 194, 225, 49, 17,
    33, 113, 65, 98, 242, 195, 161, 130, 211, 226, 50, 146, 81, 2, 34, 18, 178, 114, 66, 162, 243,
    131, 212, 196, 51, 227, 147, 3, 99, 35, 19, 82, 163, 115, 179, 244, 67, 132, 213, 197, 100, 83,
    52, 4, 148, 36, 228, 116, 20, 164, 180, 245, 214, 198, 133, 68, 101, 5, 84, 117, 53, 149, 37,
    181, 229, 21, 165, 134, 69, 215, 246, 6, 102, 85, 54, 22, 38, 150, 230, 118, 247, 182, 135, 166,
    86, 199, 103, 216, 70, 7, 55, 231, 151, 23, 119, 136, 39, 183, 217, 248, 137, 71, 167, 87, 249,
    104, 105, 56, 57, 8, 9, 200, 232, 201, 233, 24, 25, 152, 153, 40, 120, 41, 121, 184, 185, 72,
    73, 168, 88, 89, 169,
)


def plan(bits):
    if bits == len(PLAN_ORDERS[0]):
        return [list(order) for order in PLAN_ORDERS], [divmod(code, 16) for code in PLAN_STEPS]
    base = list(range(bits))
    orders = [base]
    if bits >= 3:
        a, b, c, d, e, f = [
            list(head) + base[3:]
            for head in ((0, 1, 2), (1, 0, 2), (2, 0, 1), (2, 1, 0), (0, 2, 1), (1, 2, 0))
        ]
        orders = [a, b, c, e, f, d, a, b]
    orders = [orders[g % len(orders)] for g in range(UNITS)]
    steps = [(g - UNITS, g, 0) for g in range(UNITS)]
    for g in range(UNITS):
        steps += [(g + STAGGER * i, g, i) for i in range(1, 2 * bits + 1)]
        steps.append((g + STAGGER * 2 * bits + 0.5, g, 2 * bits + 1))
    return orders, [(g, i) for _, g, i in sorted(steps)]


def permuted(index, order):
    bits = len(order)
    return sum(((index // 2**b) % 2) * 2 ** (bits - 1 - at) for at, b in enumerate(order))


def twiddles(no, lon_local, orders):
    blocks = -(-lon_local // LANES)
    period = no * lon_local

    def turn(positions):
        phase = np.outer(positions, np.arange(orders)) % period
        angle = phase * (2.0 * math.pi / period)
        return np.cos(angle), np.sin(angle)

    fine = np.concatenate(turn(np.arange(LANES)), 1)
    high = fine.astype(BF16)
    low = (fine - high.astype(np.float64)).astype(BF16)
    starts = (lon_local * np.arange(no)[:, None] + LANES * np.arange(blocks)).reshape(-1)
    cos, sin = turn(starts)
    return np.concatenate([high, low], 0), cos.astype(np.float32), sin.astype(np.float32)


def kernel(
    n, no,
    press_hbm, tables_ref, quad_hbm, love_hbm, order_hbm, cycle_hbm, fine_hbm, cos_hbm, sin_hbm,
    spec_ref, field_ref,
    tab, press_ref, quad_ref, love_ref, order_ref, cycle_ref, fine, cos_q, sin_q,
    gathered, wide, partial, orders_ref, pick, lhs, part, landed, scaled,
    natural, rotated, out_signal, in_signal,
    tab_sem, in_sem, press_sem, rs_sem, ag_sem, field_sem,
):
    bits = n.bit_length() - 1
    me = lax.axis_index("lat")
    core = lax.axis_index("ord")
    orders_of, steps = plan(bits)
    groups = len(orders_of)
    per_unit = groups // UNITS
    cycles = press_ref.shape[1]
    lon_local = press_ref.shape[2]
    local_orders = orders_ref.shape[0]
    degrees = tables_ref.shape[1]
    share = degrees // n
    go = local_orders // groups
    rows_g = go * cycles
    uo = local_orders // UNITS
    rows_u = uo * cycles
    both = 2 * cycles
    blocks = max(1, min(n, 1024 // share))
    width = blocks * share
    period = lon_local * no
    turns = cos_q.shape[0] // no
    modes = order_ref.shape[1]

    barrier = pltpu.get_barrier_semaphore()
    partners = []
    for b in range(bits):
        mine = (me // 2**b) % 2
        partners.append(me + (1 - 2 * mine) * 2**b)
    peers = [lax.rem(core + i, no) for i in range(1, no)]
    for peer in peers:
        pl.semaphore_signal(barrier, inc=1, device_id=(me, peer), device_id_type=MESH)
    for partner in partners:
        pl.semaphore_signal(barrier, inc=1, device_id=(partner, core), device_id_type=MESH)

    loads = []
    pairs = (
        (press_hbm, press_ref), (order_hbm, order_ref), (quad_hbm, quad_ref), (cycle_hbm, cycle_ref),
        (fine_hbm, fine), (cos_hbm, cos_q), (sin_hbm, sin_q), (love_hbm, love_ref),
    )
    for i, (source, to) in enumerate(pairs):
        copy = pltpu.make_async_copy(source, to, in_sem.at[i])
        copy.start()
        loads.append(copy)
    loads[0].wait()
    pl.semaphore_wait(barrier, bits + no - 1)
    press_copies = []
    for i, peer in enumerate(peers):
        copy = pltpu.make_async_remote_copy(
            src_ref=press_ref,
            dst_ref=gathered.at[i],
            send_sem=press_sem.at[0, i],
            recv_sem=press_sem.at[1, i],
            device_id=(me, peer),
            device_id_type=MESH,
        )
        copy.start()
        press_copies.append(copy)

    def widen(at, piece):
        for q in range(turns):
            first = q * LANES
            count = min(LANES, lon_local - first)
            rows = jnp.concatenate([piece[h, :, first : first + count].astype(F32) for h in range(2)], 0)
            if count < LANES:
                rows = jnp.concatenate([rows, jnp.zeros((both, LANES - count), F32)], 1)
            rows = rows.astype(BF16)
            wide[at, q * both : (q + 1) * both, :LANES] = rows
            wide[at, q * both : (q + 1) * both, LANES:] = rows

    def transform(at, origin, start):
        partial[...] = jnp.dot(wide[at], fine[...], preferred_element_type=F32)

        cos_sum, sin_sum = start
        for q in range(turns):
            rows = slice(q * both, (q + 1) * both)
            c = partial[rows, :modes]
            s = partial[rows, modes:]
            cq = cos_q[pl.ds(origin * turns + q, 1), :]
            sq = sin_q[pl.ds(origin * turns + q, 1), :]
            cos_sum = cos_sum + (cq * c - sq * s)
            sin_sum = sin_sum + (sq * c + cq * s)
        return cos_sum, sin_sum

    widen(0, press_ref)
    for copy in loads[1:]:
        copy.wait()
    tab_copies = []
    for u in range(UNITS):
        rows = pl.ds(u * rows_u, rows_u)
        copy = pltpu.make_async_copy(tables_ref.at[rows], tab.at[rows], tab_sem.at[u])
        copy.start()
        tab_copies.append(copy)
    shape = (local_orders, modes)
    slot = core * local_orders + lax.broadcasted_iota(jnp.int32, shape, 0)
    lane = lax.broadcasted_iota(jnp.int32, shape, 1)
    order_col = jnp.sum(
        jnp.where(slot == lane, order_ref[...].astype(F32), 0.0), axis=1, keepdims=True
    ).astype(jnp.int32)
    orders_ref[...] = order_col
    pick[...] = jnp.where(order_col == lane, 1.0, 0.0).astype(BF16)

    square = (cycles, cycles)
    eye = lax.broadcasted_iota(jnp.int32, square, 0) == lax.broadcasted_iota(jnp.int32, square, 1)
    cycle_col = jnp.sum(
        jnp.where(eye, cycle_ref[...].astype(F32), 0.0), axis=1, keepdims=True
    ).astype(jnp.int32)
    quad_lane = lax.broadcasted_iota(jnp.int32, (cycles, quad_ref.shape[1]), 1)
    weight = jnp.sum(jnp.where(quad_lane == cycle_col, quad_ref[...], 0.0), axis=1, keepdims=True)
    weight = weight * (1.0 / math.sqrt(quad_ref.shape[1])) * (1.0 / math.sqrt(period))

    col = lax.broadcasted_iota(jnp.int32, (uo, rows_u), 1) // cycles
    row = lax.broadcasted_iota(jnp.int32, (uo, rows_u), 0)
    diagonal = row == col
    spread_row = lax.broadcasted_iota(jnp.int32, (4 * cycles, 4 * rows_u), 0)
    spread_col = lax.broadcasted_iota(jnp.int32, (4 * cycles, 4 * rows_u), 1)
    spread = jnp.where(
        spread_row == (spread_col // rows_u) * cycles + spread_col % cycles, 1.0, 0.0
    ).astype(BF16)
    lane_order = lax.broadcasted_iota(jnp.int32, (cycles, 4 * go), 1) % go
    lane_part = lax.broadcasted_iota(jnp.int32, (cycles, 4 * go), 1) // go

    zero = jnp.zeros((both, modes), F32)
    sums = transform(0, core, (zero, zero))
    for i, copy in enumerate(press_copies):
        copy.wait()
        widen(i + 1, gathered.at[i])
        sums = transform(i + 1, lax.rem(core + no - 1 - i, no), sums)
    cos_sum, sin_sum = sums
    folded = jnp.concatenate(
        [
            weight * (cos_sum[:cycles] + cos_sum[cycles:]),
            -weight * (sin_sum[:cycles] + sin_sum[cycles:]),
            weight * (cos_sum[:cycles] - cos_sum[cycles:]),
            -weight * (sin_sum[:cycles] - sin_sum[cycles:]),
        ],
        0,
    ).astype(BF16)
    chosen = lax.dot_general(pick[...], folded, NT, preferred_element_type=F32).astype(BF16)
    repeated = jnp.dot(chosen, spread, preferred_element_type=F32)
    for u in range(UNITS):
        rows = repeated[u * uo : (u + 1) * uo]
        lhs[u] = jnp.concatenate(
            [jnp.where(diagonal, rows[:, c * rows_u : (c + 1) * rows_u], 0.0) for c in range(4)], 0
        ).astype(BF16)

    def parity(start, count, first):
        degree = first + lax.broadcasted_iota(jnp.int32, (count, width), 1)
        order = orders_ref[start : start + count, :]
        return (degree + order) & 1 == 0, degree >= order

    def region(g, k):
        base = 0
        for at in range(k):
            base = base + ((me // 2 ** orders_of[g][at]) % 2) * (n >> (at + 1))
        return base

    def analyse(u):
        tab_copies[u].wait()
        left = lhs[u]
        for i in range(degrees // width):
            first = i * width
            product = jnp.dot(
                left, tab[u * rows_u : (u + 1) * rows_u, first : first + width],
                preferred_element_type=F32,
            )
            even, present = parity(u * uo, uo, first)
            real = jnp.where(present, jnp.where(even, product[:uo], product[2 * uo : 3 * uo]), 0.0)
            imag = jnp.where(present, jnp.where(even, product[uo : 2 * uo], product[3 * uo :]), 0.0)
            for v in range(per_unit):
                g = u * per_unit + v
                rows = slice(v * go, (v + 1) * go)
                value = jnp.concatenate([real[rows], imag[rows]], 0).astype(BF16)
                for j in range(blocks):
                    to = permuted(i * blocks + j, orders_of[g])
                    part[g, to] = value[:, j * share : (j + 1) * share]

    reduce_copies = {}
    gather_copies = {}

    def send_reduce(g, k):
        h = n >> (k + 1)
        b = orders_of[g][k]
        mine = (me // 2**b) % 2
        copy = pltpu.make_async_remote_copy(
            src_ref=part.at[g, pl.ds(region(g, k) + (1 - mine) * h, h)],
            dst_ref=landed.at[g, pl.ds(n - (n >> k), h)],
            send_sem=rs_sem.at[0, g, k],
            recv_sem=rs_sem.at[1, g, k],
            device_id=(partners[b], core),
            device_id_type=MESH,
        )
        copy.start()
        reduce_copies[g, k] = copy

    def take_reduce(g, k):
        h = n >> (k + 1)
        reduce_copies[g, k].wait_recv()
        keep = region(g, k + 1)
        off = n - (n >> k)
        if k < bits - 1:

            def add(i, carry):
                part[g, keep + i] = (
                    part[g, keep + i].astype(F32) + landed[g, off + i].astype(F32)
                ).astype(BF16)
                return carry

            lax.fori_loop(0, h, add, 0, unroll=min(h, 4))
            send_reduce(g, k + 1)
            return
        total = part[g, keep].astype(F32) + landed[g, off].astype(F32)
        spec_ref[0, g * go : (g + 1) * go, :] = total[:go]
        spec_ref[1, g * go : (g + 1) * go, :] = total[go:]
        scaled[g, keep] = (DENSITY_RATIO * (1.0 + love_ref[pl.ds(me, 1), :]) * total).astype(BF16)
        send_gather(g, bits - 1)

    def send_gather(g, k):
        h = n >> (k + 1)
        b = orders_of[g][k]
        mine = pl.ds(region(g, k + 1), h)
        copy = pltpu.make_async_remote_copy(
            src_ref=scaled.at[g, mine],
            dst_ref=scaled.at[g, mine],
            send_sem=ag_sem.at[0, g, k],
            recv_sem=ag_sem.at[1, g, k],
            device_id=(partners[b], core),
            device_id_type=MESH,
        )
        copy.start()
        gather_copies[g, k] = copy

    def take_gather(g, k):
        gather_copies[g, k].wait_recv()
        if k > 0:
            send_gather(g, k - 1)

    def synthesise(g):
        total = jnp.zeros((rows_g, 4 * go), F32)
        for i in range(degrees // width):
            first = i * width
            even, _ = parity(g * go, go, first)
            pieces = [scaled[g, permuted(i * blocks + j, orders_of[g])] for j in range(blocks)]
            both_parts = jnp.concatenate(pieces, 1).astype(F32)
            real, imag = both_parts[:go], both_parts[go:]
            stacked = jnp.concatenate(
                [real, imag, jnp.where(even, real, -real), jnp.where(even, imag, -imag)], 0
            ).astype(BF16)
            total = total + lax.dot_general(
                tab[g * rows_g : (g + 1) * rows_g, first : first + width], stacked, NT,
                preferred_element_type=F32,
            )
        signal = jnp.zeros((cycles, 4 * go), F32)
        for o in range(go):
            signal = jnp.where(lane_order == o, total[o * cycles : (o + 1) * cycles], signal)
        signal = signal * (1.0 / math.sqrt(degrees))
        split = jnp.concatenate([jnp.where(lane_part == c, signal, 0.0) for c in range(4)], 0)
        chosen_rows = jnp.concatenate([pick[g * go : (g + 1) * go, :]] * 4, 0)
        piece = jnp.dot(split.astype(BF16), chosen_rows, preferred_element_type=F32)
        natural[...] += piece

    natural[...] = jnp.zeros_like(natural)
    for g, i in steps:
        if i == 0:
            analyse(g // per_unit)
            for v in range(per_unit):
                send_reduce(g + v, 0)
        elif i <= bits:
            take_reduce(g, i - 1)
        elif i <= 2 * bits:
            take_gather(g, 2 * bits - i)
        else:
            synthesise(g)

    out_signal[...] = natural[...].astype(BF16)
    field_copies = []
    for i, peer in enumerate(peers):
        copy = pltpu.make_async_remote_copy(
            src_ref=out_signal,
            dst_ref=in_signal.at[i],
            send_sem=field_sem.at[0, i],
            recv_sem=field_sem.at[1, i],
            device_id=(me, peer),
            device_id_type=MESH,
        )
        copy.start()
        field_copies.append(copy)
    total = out_signal[...].astype(F32)
    for i, copy in enumerate(field_copies):
        copy.wait_recv()
        total = total + in_signal[i].astype(F32)
    total = total * (1.0 / math.sqrt(modes))
    real = jnp.concatenate([total[:cycles], total[2 * cycles : 3 * cycles]], 0)
    imag = jnp.concatenate([total[cycles : 2 * cycles], total[3 * cycles :]], 0)
    for q in range(turns):
        cq = cos_q[pl.ds(core * turns + q, 1), :]
        sq = sin_q[pl.ds(core * turns + q, 1), :]
        rows = slice(q * both, (q + 1) * both)
        rotated[rows, :modes] = (real * cq - imag * sq).astype(BF16)
        rotated[rows, modes:] = (-real * sq - imag * cq).astype(BF16)
    parts = lax.dot_general(rotated[...], fine[...], NT, preferred_element_type=F32)
    field = parts[:, :LANES] + parts[:, LANES:]
    for q in range(turns):
        first = q * LANES
        count = min(LANES, lon_local - first)
        for h in range(2):
            at = q * both + h * cycles
            field_ref[h, :, first : first + count] = field[at : at + cycles, :count]
    for copy in list(reduce_copies.values()) + list(gather_copies.values()) + field_copies:
        copy.wait_send()


def finish(half_spec, half_field, spec_ref, field_ref):
    spec_ref[...] = half_spec[...]
    field_ref[...] = half_field[...]


def per_device(n, no, pressure, tables, quad_weight, love_number, order_list, cycle_list):
    _, cycles, lon_local = pressure.shape
    local_orders, _, degrees = tables.shape
    bits = n.bit_length() - 1
    share = degrees // n
    groups = len(plan(bits)[0])
    go = local_orders // groups
    uo = local_orders // UNITS
    modes = order_list.shape[0]
    turns = -(-lon_local // LANES)
    fine, cos_q, sin_q = [jnp.asarray(table) for table in twiddles(no, lon_local, modes)]
    small = (
        quad_weight[None, :], love_number.reshape(n, share), order_list[None, :], cycle_list[None, :],
        fine, cos_q, sin_q,
    )
    vmem = pl.BlockSpec(memory_space=pltpu.VMEM)
    hbm = pl.BlockSpec(memory_space=pl.ANY)
    blocks = pltpu.VMEM((groups, n, 2 * go, share), BF16)
    spectrum, field = pl.pallas_call(
        functools.partial(kernel, n, no),
        out_shape=(
            jax.ShapeDtypeStruct((2, local_orders, share), F32),
            jax.ShapeDtypeStruct((2, cycles, lon_local), F32),
        ),
        in_specs=[hbm] * 9,
        out_specs=(vmem, vmem),
        scratch_shapes=[
            pltpu.VMEM((local_orders * cycles, degrees), BF16),
            pltpu.VMEM((2, cycles, lon_local), BF16),
            *[pltpu.VMEM(array.shape, array.dtype) for array in small],
            pltpu.VMEM((no - 1, 2, cycles, lon_local), BF16),
            pltpu.VMEM((no, turns * 2 * cycles, 2 * LANES), BF16),
            pltpu.VMEM((turns * 2 * cycles, 2 * modes), F32),
            pltpu.VMEM((local_orders, 1), jnp.int32),
            pltpu.VMEM((local_orders, modes), BF16),
            pltpu.VMEM((UNITS, 4 * uo, uo * cycles), BF16),
            blocks, blocks, blocks,
            pltpu.VMEM((4 * cycles, modes), F32),
            pltpu.VMEM((turns * 2 * cycles, 2 * modes), BF16),
            pltpu.VMEM((4 * cycles, modes), BF16),
            pltpu.VMEM((no - 1, 4 * cycles, modes), BF16),
            pltpu.SemaphoreType.DMA((UNITS,)),
            pltpu.SemaphoreType.DMA((8,)),
            pltpu.SemaphoreType.DMA((2, no - 1)),
            pltpu.SemaphoreType.DMA((2, groups, bits)),
            pltpu.SemaphoreType.DMA((2, groups, bits)),
            pltpu.SemaphoreType.DMA((2, no - 1)),
        ],
        compiler_params=pltpu.CompilerParams(
            collective_id=0, has_side_effects=True, vmem_limit_bytes=56 * 1024 * 1024
        ),
    )(pressure, tables.reshape(local_orders * cycles, degrees), *small)
    return pl.pallas_call(
        finish,
        out_shape=(
            jax.ShapeDtypeStruct(spectrum.shape, F32),
            jax.ShapeDtypeStruct(field.shape, F32),
        ),
        in_specs=[vmem, vmem],
        out_specs=(vmem, vmem),
    )(spectrum, field)


def solution(mesh):
    placed = (P(None, "lat", "ord"), P("ord", "lat", None), P(), P(), P(), P("lat"))
    return jax.shard_map(
        functools.partial(per_device, mesh.shape["lat"], mesh.shape["ord"]),
        mesh=mesh,
        in_specs=placed,
        out_specs=(P(None, "ord", "lat"), P(None, "lat", "ord")),
        check_vma=False,
    )
```

```python
import functools
import math

import jax
import jax.numpy as jnp
import numpy as np
from jax import lax
from jax.experimental import pallas as pl
from jax.experimental.pallas import tpu as pltpu
from jax.sharding import PartitionSpec as P

DENSITY_RATIO = 3.0 * 1025.0 / 5517.0
LANES = 128
UNITS = 8
STAGGER = 4
MESH = pl.DeviceIdType.MESH
NT = (((1,), (1,)), ((), ()))
F32 = jnp.float32
BF16 = jnp.bfloat16


PLAN_ORDERS = (
    (1, 0, 2, 3), (2, 0, 1, 3), (2, 0, 3, 1), (0, 2, 1, 3), (2, 3, 1, 0), (0, 1, 2, 3),
    (0, 1, 2, 3), (1, 0, 2, 3), (0, 1, 2, 3), (1, 0, 2, 3), (2, 1, 0, 3), (2, 0, 1, 3),
    (2, 1, 0, 3), (1, 0, 2, 3), (0, 1, 2, 3), (1, 3, 2, 0),
)
PLAN_STEPS = (
    32, 224, 128, 160, 192, 225, 145, 161, 64, 129, 49, 209, 96, 226, 241, 33, 146, 0, 130, 210, 65,
    193, 81, 50, 162, 97, 177, 227, 113, 34, 1, 147, 163, 131, 17, 194, 242, 82, 98, 114, 211, 66,
    228, 178, 35, 51, 2, 195, 164, 18, 243, 83, 132, 67, 148, 115, 179, 99, 212, 229, 244, 52, 3,
    19, 196, 165, 84, 133, 149, 36, 116, 68, 100, 230, 180, 213, 245, 20, 4, 197, 53, 37, 85, 134,
    150, 117, 69, 101, 166, 181, 214, 231, 246, 198, 5, 21, 54, 86, 38, 135, 70, 102, 167, 118, 215,
    182, 247, 199, 6, 151, 22, 232, 233, 55, 39, 87, 71, 103, 136, 137, 216, 119, 217, 183, 168,
    169, 248, 7, 249, 23, 200, 201, 152, 153, 56, 57, 40, 41, 88, 89, 72, 73, 104, 105, 120, 121,
    184, 185, 8, 9, 24, 25,
)


def plan(bits):
    if bits == len(PLAN_ORDERS[0]):
        return [list(order) for order in PLAN_ORDERS], [divmod(code, 16) for code in PLAN_STEPS]
    base = list(range(bits))
    orders = [base]
    if bits >= 3:
        a, b, c, d, e, f = [
            list(head) + base[3:]
            for head in ((0, 1, 2), (1, 0, 2), (2, 0, 1), (2, 1, 0), (0, 2, 1), (1, 2, 0))
        ]
        orders = [a, b, c, e, f, d, a, b]
    orders = [orders[g % len(orders)] for g in range(UNITS)]
    steps = [(g - UNITS, g, 0) for g in range(UNITS)]
    for g in range(UNITS):
        steps += [(g + STAGGER * i, g, i) for i in range(1, 2 * bits + 1)]
        steps.append((g + STAGGER * 2 * bits + 0.5, g, 2 * bits + 1))
    return orders, [(g, i) for _, g, i in sorted(steps)]


def permuted(index, order):
    bits = len(order)
    return sum(((index // 2**b) % 2) * 2 ** (bits - 1 - at) for at, b in enumerate(order))


def twiddles(no, lon_local, orders):
    blocks = -(-lon_local // LANES)
    period = no * lon_local

    def turn(positions):
        phase = np.outer(positions, np.arange(orders)) % period
        angle = phase * (2.0 * math.pi / period)
        return np.cos(angle), np.sin(angle)

    fine = np.concatenate(turn(np.arange(LANES)), 1)
    high = fine.astype(BF16)
    low = (fine - high.astype(np.float64)).astype(BF16)
    starts = (lon_local * np.arange(no)[:, None] + LANES * np.arange(blocks)).reshape(-1)
    cos, sin = turn(starts)
    return np.concatenate([high, low], 0), cos.astype(np.float32), sin.astype(np.float32)


def kernel(
    n, no,
    press_hbm, tables_ref, quad_hbm, love_hbm, order_hbm, cycle_hbm, fine_hbm, cos_hbm, sin_hbm,
    spec_ref, field_ref,
    tab, press_ref, quad_ref, love_ref, order_ref, cycle_ref, fine, cos_q, sin_q,
    gathered, wide, partial, orders_ref, pick, lhs, part, landed, scaled,
    signals, rotated, out_signal, in_signal,
    tab_sem, in_sem, press_sem, rs_sem, ag_sem, field_sem,
):
    bits = n.bit_length() - 1
    me = lax.axis_index("lat")
    core = lax.axis_index("ord")
    orders_of, steps = plan(bits)
    groups = len(orders_of)
    per_unit = groups // UNITS
    cycles = press_ref.shape[1]
    lon_local = press_ref.shape[2]
    local_orders = orders_ref.shape[0]
    degrees = tables_ref.shape[1]
    share = degrees // n
    go = local_orders // groups
    rows_g = go * cycles
    uo = local_orders // UNITS
    rows_u = uo * cycles
    both = 2 * cycles
    blocks = max(1, min(n, 1024 // share))
    width = blocks * share
    period = lon_local * no
    turns = cos_q.shape[0] // no
    modes = order_ref.shape[1]

    barrier = pltpu.get_barrier_semaphore()
    partners = []
    for b in range(bits):
        mine = (me // 2**b) % 2
        partners.append(me + (1 - 2 * mine) * 2**b)
    peers = [lax.rem(core + i, no) for i in range(1, no)]
    for peer in peers:
        pl.semaphore_signal(barrier, inc=1, device_id=(me, peer), device_id_type=MESH)
    for partner in partners:
        pl.semaphore_signal(barrier, inc=1, device_id=(partner, core), device_id_type=MESH)

    loads = []
    pairs = (
        (press_hbm, press_ref), (order_hbm, order_ref), (quad_hbm, quad_ref), (cycle_hbm, cycle_ref),
        (fine_hbm, fine), (cos_hbm, cos_q), (sin_hbm, sin_q), (love_hbm, love_ref),
    )
    for i, (source, to) in enumerate(pairs):
        copy = pltpu.make_async_copy(source, to, in_sem.at[i])
        copy.start()
        loads.append(copy)
    loads[0].wait()
    pl.semaphore_wait(barrier, bits + no - 1)
    press_copies = []
    for i, peer in enumerate(peers):
        copy = pltpu.make_async_remote_copy(
            src_ref=press_ref,
            dst_ref=gathered.at[i],
            send_sem=press_sem.at[0, i],
            recv_sem=press_sem.at[1, i],
            device_id=(me, peer),
            device_id_type=MESH,
        )
        copy.start()
        press_copies.append(copy)

    def widen(at, piece):
        for q in range(turns):
            first = q * LANES
            count = min(LANES, lon_local - first)
            rows = jnp.concatenate([piece[h, :, first : first + count].astype(F32) for h in range(2)], 0)
            if count < LANES:
                rows = jnp.concatenate([rows, jnp.zeros((both, LANES - count), F32)], 1)
            rows = rows.astype(BF16)
            wide[at, q * both : (q + 1) * both, :LANES] = rows
            wide[at, q * both : (q + 1) * both, LANES:] = rows

    def transform(at, origin, start):
        partial[...] = jnp.dot(wide[at], fine[...], preferred_element_type=F32)

        cos_sum, sin_sum = start
        for q in range(turns):
            rows = slice(q * both, (q + 1) * both)
            c = partial[rows, :modes]
            s = partial[rows, modes:]
            cq = cos_q[pl.ds(origin * turns + q, 1), :]
            sq = sin_q[pl.ds(origin * turns + q, 1), :]
            cos_sum = cos_sum + (cq * c - sq * s)
            sin_sum = sin_sum + (sq * c + cq * s)
        return cos_sum, sin_sum

    widen(0, press_ref)
    for copy in loads[1:]:
        copy.wait()
    tab_copies = {}
    for u in [g // per_unit for g, i in steps if i == 0]:
        rows = pl.ds(u * rows_u, rows_u)
        copy = pltpu.make_async_copy(tables_ref.at[rows], tab.at[rows], tab_sem.at[u])
        copy.start()
        tab_copies[u] = copy
    shape = (local_orders, modes)
    slot = core * local_orders + lax.broadcasted_iota(jnp.int32, shape, 0)
    lane = lax.broadcasted_iota(jnp.int32, shape, 1)
    order_col = jnp.sum(
        jnp.where(slot == lane, order_ref[...].astype(F32), 0.0), axis=1, keepdims=True
    ).astype(jnp.int32)
    orders_ref[...] = order_col
    pick[...] = jnp.where(order_col == lane, 1.0, 0.0).astype(BF16)

    square = (cycles, cycles)
    eye = lax.broadcasted_iota(jnp.int32, square, 0) == lax.broadcasted_iota(jnp.int32, square, 1)
    cycle_col = jnp.sum(
        jnp.where(eye, cycle_ref[...].astype(F32), 0.0), axis=1, keepdims=True
    ).astype(jnp.int32)
    quad_lane = lax.broadcasted_iota(jnp.int32, (cycles, quad_ref.shape[1]), 1)
    weight = jnp.sum(jnp.where(quad_lane == cycle_col, quad_ref[...], 0.0), axis=1, keepdims=True)
    weight = weight * (1.0 / math.sqrt(quad_ref.shape[1])) * (1.0 / math.sqrt(period))

    col = lax.broadcasted_iota(jnp.int32, (uo, rows_u), 1) // cycles
    row = lax.broadcasted_iota(jnp.int32, (uo, rows_u), 0)
    diagonal = row == col
    spread_row = lax.broadcasted_iota(jnp.int32, (4 * cycles, 4 * rows_u), 0)
    spread_col = lax.broadcasted_iota(jnp.int32, (4 * cycles, 4 * rows_u), 1)
    spread = jnp.where(
        spread_row == (spread_col // rows_u) * cycles + spread_col % cycles, 1.0, 0.0
    ).astype(BF16)
    lane_order = lax.broadcasted_iota(jnp.int32, (cycles, 4 * go), 1) % go

    zero = jnp.zeros((both, modes), F32)
    sums = transform(0, core, (zero, zero))
    for i, copy in enumerate(press_copies):
        copy.wait()
        widen(i + 1, gathered.at[i])
        sums = transform(i + 1, lax.rem(core + no - 1 - i, no), sums)
    cos_sum, sin_sum = sums
    folded = jnp.concatenate(
        [
            weight * (cos_sum[:cycles] + cos_sum[cycles:]),
            -weight * (sin_sum[:cycles] + sin_sum[cycles:]),
            weight * (cos_sum[:cycles] - cos_sum[cycles:]),
            -weight * (sin_sum[:cycles] - sin_sum[cycles:]),
        ],
        0,
    ).astype(BF16)
    chosen = lax.dot_general(pick[...], folded, NT, preferred_element_type=F32).astype(BF16)
    repeated = jnp.dot(chosen, spread, preferred_element_type=F32)
    for u in range(UNITS):
        rows = repeated[u * uo : (u + 1) * uo]
        lhs[u] = jnp.concatenate(
            [jnp.where(diagonal, rows[:, c * rows_u : (c + 1) * rows_u], 0.0) for c in range(4)], 0
        ).astype(BF16)

    def parity(start, count, first):
        degree = first + lax.broadcasted_iota(jnp.int32, (count, width), 1)
        order = orders_ref[start : start + count, :]
        return (degree + order) & 1 == 0, degree >= order

    def region(g, k):
        base = 0
        for at in range(k):
            base = base + ((me // 2 ** orders_of[g][at]) % 2) * (n >> (at + 1))
        return base

    def analyse(u):
        tab_copies[u].wait()
        left = lhs[u]
        for i in range(degrees // width):
            first = i * width
            product = jnp.dot(
                left, tab[u * rows_u : (u + 1) * rows_u, first : first + width],
                preferred_element_type=F32,
            )
            even, present = parity(u * uo, uo, first)
            real = jnp.where(present, jnp.where(even, product[:uo], product[2 * uo : 3 * uo]), 0.0)
            imag = jnp.where(present, jnp.where(even, product[uo : 2 * uo], product[3 * uo :]), 0.0)
            for v in range(per_unit):
                g = u * per_unit + v
                rows = slice(v * go, (v + 1) * go)
                value = jnp.concatenate([real[rows], imag[rows]], 0).astype(BF16)
                for j in range(blocks):
                    to = permuted(i * blocks + j, orders_of[g])
                    part[g, to] = value[:, j * share : (j + 1) * share]

    reduce_copies = {}
    gather_copies = {}

    def send_reduce(g, k):
        h = n >> (k + 1)
        b = orders_of[g][k]
        mine = (me // 2**b) % 2
        copy = pltpu.make_async_remote_copy(
            src_ref=part.at[g, pl.ds(region(g, k) + (1 - mine) * h, h)],
            dst_ref=landed.at[g, pl.ds(n - (n >> k), h)],
            send_sem=rs_sem.at[0, g, k],
            recv_sem=rs_sem.at[1, g, k],
            device_id=(partners[b], core),
            device_id_type=MESH,
        )
        copy.start()
        reduce_copies[g, k] = copy

    def take_reduce(g, k):
        h = n >> (k + 1)
        reduce_copies[g, k].wait_recv()
        keep = region(g, k + 1)
        off = n - (n >> k)
        if k < bits - 1:

            def add(i, carry):
                part[g, keep + i] = (
                    part[g, keep + i].astype(F32) + landed[g, off + i].astype(F32)
                ).astype(BF16)
                return carry

            lax.fori_loop(0, h, add, 0, unroll=min(h, 4))
            send_reduce(g, k + 1)
            return
        total = part[g, keep].astype(F32) + landed[g, off].astype(F32)
        spec_ref[0, g * go : (g + 1) * go, :] = total[:go]
        spec_ref[1, g * go : (g + 1) * go, :] = total[go:]
        scaled[g, keep] = (DENSITY_RATIO * (1.0 + love_ref[pl.ds(me, 1), :]) * total).astype(BF16)
        send_gather(g, bits - 1)

    def send_gather(g, k):
        h = n >> (k + 1)
        b = orders_of[g][k]
        mine = pl.ds(region(g, k + 1), h)
        copy = pltpu.make_async_remote_copy(
            src_ref=scaled.at[g, mine],
            dst_ref=scaled.at[g, mine],
            send_sem=ag_sem.at[0, g, k],
            recv_sem=ag_sem.at[1, g, k],
            device_id=(partners[b], core),
            device_id_type=MESH,
        )
        copy.start()
        gather_copies[g, k] = copy

    def take_gather(g, k):
        gather_copies[g, k].wait_recv()
        if k > 0:
            send_gather(g, k - 1)

    def synthesise(g):
        total = jnp.zeros((rows_g, 4 * go), F32)
        for i in range(degrees // width):
            first = i * width
            even, _ = parity(g * go, go, first)
            pieces = [scaled[g, permuted(i * blocks + j, orders_of[g])] for j in range(blocks)]
            both_parts = jnp.concatenate(pieces, 1).astype(F32)
            real, imag = both_parts[:go], both_parts[go:]
            stacked = jnp.concatenate(
                [real, imag, jnp.where(even, real, -real), jnp.where(even, imag, -imag)], 0
            ).astype(BF16)
            total = total + lax.dot_general(
                tab[g * rows_g : (g + 1) * rows_g, first : first + width], stacked, NT,
                preferred_element_type=F32,
            )
        signal = jnp.zeros((cycles, 4 * go), F32)
        for o in range(go):
            signal = jnp.where(lane_order == o, total[o * cycles : (o + 1) * cycles], signal)
        signal = signal * (1.0 / math.sqrt(degrees))
        for c in range(4):
            signals[c * cycles : (c + 1) * cycles, g * go : (g + 1) * go] = signal[:, c * go : (c + 1) * go]

    for g, i in steps:
        if i == 0:
            analyse(g // per_unit)
            for v in range(per_unit):
                send_reduce(g + v, 0)
        elif i <= bits:
            take_reduce(g, i - 1)
        elif i <= 2 * bits:
            take_gather(g, 2 * bits - i)
        else:
            synthesise(g)

    natural = jnp.dot(signals[...].astype(BF16), pick[...], preferred_element_type=F32)
    out_signal[...] = natural.astype(BF16)
    field_copies = []
    for i, peer in enumerate(peers):
        copy = pltpu.make_async_remote_copy(
            src_ref=out_signal,
            dst_ref=in_signal.at[i],
            send_sem=field_sem.at[0, i],
            recv_sem=field_sem.at[1, i],
            device_id=(me, peer),
            device_id_type=MESH,
        )
        copy.start()
        field_copies.append(copy)
    total = natural
    for i, copy in enumerate(field_copies):
        copy.wait_recv()
        total = total + in_signal[i].astype(F32)
    total = total * (1.0 / math.sqrt(modes))
    real = jnp.concatenate([total[:cycles], total[2 * cycles : 3 * cycles]], 0)
    imag = jnp.concatenate([total[cycles : 2 * cycles], total[3 * cycles :]], 0)
    for q in range(turns):
        cq = cos_q[pl.ds(core * turns + q, 1), :]
        sq = sin_q[pl.ds(core * turns + q, 1), :]
        rows = slice(q * both, (q + 1) * both)
        rotated[rows, :modes] = (real * cq - imag * sq).astype(BF16)
        rotated[rows, modes:] = (-real * sq - imag * cq).astype(BF16)
    parts = lax.dot_general(rotated[...], fine[...], NT, preferred_element_type=F32)
    field = parts[:, :LANES] + parts[:, LANES:]
    for q in range(turns):
        first = q * LANES
        count = min(LANES, lon_local - first)
        for h in range(2):
            at = q * both + h * cycles
            field_ref[h, :, first : first + count] = field[at : at + cycles, :count]
    for copy in list(reduce_copies.values()) + list(gather_copies.values()) + field_copies:
        copy.wait_send()


def finish(half_spec, half_field, spec_ref, field_ref):
    spec_ref[...] = half_spec[...]
    field_ref[...] = half_field[...]


def per_device(n, no, pressure, tables, quad_weight, love_number, order_list, cycle_list):
    _, cycles, lon_local = pressure.shape
    local_orders, _, degrees = tables.shape
    bits = n.bit_length() - 1
    share = degrees // n
    groups = len(plan(bits)[0])
    go = local_orders // groups
    uo = local_orders // UNITS
    modes = order_list.shape[0]
    turns = -(-lon_local // LANES)
    fine, cos_q, sin_q = [jnp.asarray(table) for table in twiddles(no, lon_local, modes)]
    small = (
        quad_weight[None, :], love_number.reshape(n, share), order_list[None, :], cycle_list[None, :],
        fine, cos_q, sin_q,
    )
    vmem = pl.BlockSpec(memory_space=pltpu.VMEM)
    hbm = pl.BlockSpec(memory_space=pl.ANY)
    blocks = pltpu.VMEM((groups, n, 2 * go, share), BF16)
    spectrum, field = pl.pallas_call(
        functools.partial(kernel, n, no),
        out_shape=(
            jax.ShapeDtypeStruct((2, local_orders, share), F32),
            jax.ShapeDtypeStruct((2, cycles, lon_local), F32),
        ),
        in_specs=[hbm] * 9,
        out_specs=(vmem, vmem),
        scratch_shapes=[
            pltpu.VMEM((local_orders * cycles, degrees), BF16),
            pltpu.VMEM((2, cycles, lon_local), BF16),
            *[pltpu.VMEM(array.shape, array.dtype) for array in small],
            pltpu.VMEM((no - 1, 2, cycles, lon_local), BF16),
            pltpu.VMEM((no, turns * 2 * cycles, 2 * LANES), BF16),
            pltpu.VMEM((turns * 2 * cycles, 2 * modes), F32),
            pltpu.VMEM((local_orders, 1), jnp.int32),
            pltpu.VMEM((local_orders, modes), BF16),
            pltpu.VMEM((UNITS, 4 * uo, uo * cycles), BF16),
            blocks, blocks, blocks,
            pltpu.VMEM((4 * cycles, local_orders), F32),
            pltpu.VMEM((turns * 2 * cycles, 2 * modes), BF16),
            pltpu.VMEM((4 * cycles, modes), BF16),
            pltpu.VMEM((no - 1, 4 * cycles, modes), BF16),
            pltpu.SemaphoreType.DMA((UNITS,)),
            pltpu.SemaphoreType.DMA((8,)),
            pltpu.SemaphoreType.DMA((2, no - 1)),
            pltpu.SemaphoreType.DMA((2, groups, bits)),
            pltpu.SemaphoreType.DMA((2, groups, bits)),
            pltpu.SemaphoreType.DMA((2, no - 1)),
        ],
        compiler_params=pltpu.CompilerParams(
            collective_id=0, has_side_effects=True, vmem_limit_bytes=56 * 1024 * 1024
        ),
    )(pressure, tables.reshape(local_orders * cycles, degrees), *small)
    return pl.pallas_call(
        finish,
        out_shape=(
            jax.ShapeDtypeStruct(spectrum.shape, F32),
            jax.ShapeDtypeStruct(field.shape, F32),
        ),
        in_specs=[vmem, vmem],
        out_specs=(vmem, vmem),
    )(spectrum, field)


def solution(mesh):
    placed = (P(None, "lat", "ord"), P("ord", "lat", None), P(), P(), P(), P("lat"))
    return jax.shard_map(
        functools.partial(per_device, mesh.shape["lat"], mesh.shape["ord"]),
        mesh=mesh,
        in_specs=placed,
        out_specs=(P(None, "ord", "lat"), P(None, "lat", "ord")),
        check_vma=False,
    )
```

```python
import functools
import math

import jax
import jax.numpy as jnp
import numpy as np
from jax import lax
from jax.experimental import pallas as pl
from jax.experimental.pallas import tpu as pltpu
from jax.sharding import PartitionSpec as P

DENSITY_RATIO = 3.0 * 1025.0 / 5517.0
LANES = 128
UNITS = 8
STAGGER = 4
MESH = pl.DeviceIdType.MESH
NT = (((1,), (1,)), ((), ()))
F32 = jnp.float32
BF16 = jnp.bfloat16


PLAN_ORDERS = (
    (1, 0, 2, 3), (2, 0, 1, 3), (2, 0, 3, 1), (0, 2, 1, 3), (2, 3, 1, 0), (0, 1, 2, 3),
    (0, 1, 2, 3), (1, 0, 2, 3), (0, 1, 2, 3), (1, 0, 2, 3), (2, 1, 0, 3), (2, 0, 1, 3),
    (2, 1, 0, 3), (1, 0, 2, 3), (0, 1, 2, 3), (1, 3, 2, 0),
)
PLAN_STEPS = (
    32, 224, 128, 160, 192, 225, 145, 161, 64, 129, 49, 209, 96, 226, 241, 33, 146, 0, 130, 210, 65,
    193, 81, 50, 162, 97, 177, 227, 113, 34, 1, 147, 163, 131, 17, 194, 242, 82, 98, 114, 211, 66,
    228, 178, 35, 51, 2, 195, 164, 18, 243, 83, 132, 67, 148, 115, 179, 99, 212, 229, 244, 52, 3,
    19, 196, 165, 84, 133, 149, 36, 116, 68, 100, 230, 180, 213, 245, 20, 4, 197, 53, 37, 85, 134,
    150, 117, 69, 101, 166, 181, 214, 231, 246, 198, 5, 21, 54, 86, 38, 135, 70, 102, 167, 118, 215,
    182, 247, 199, 6, 151, 22, 232, 233, 55, 39, 87, 71, 103, 136, 137, 216, 119, 217, 183, 168,
    169, 248, 7, 249, 23, 200, 201, 152, 153, 56, 57, 40, 41, 88, 89, 72, 73, 104, 105, 120, 121,
    184, 185, 8, 9, 24, 25,
)


def plan(bits):
    if bits == len(PLAN_ORDERS[0]):
        return [list(order) for order in PLAN_ORDERS], [divmod(code, 16) for code in PLAN_STEPS]
    base = list(range(bits))
    orders = [base]
    if bits >= 3:
        a, b, c, d, e, f = [
            list(head) + base[3:]
            for head in ((0, 1, 2), (1, 0, 2), (2, 0, 1), (2, 1, 0), (0, 2, 1), (1, 2, 0))
        ]
        orders = [a, b, c, e, f, d, a, b]
    orders = [orders[g % len(orders)] for g in range(UNITS)]
    steps = [(g - UNITS, g, 0) for g in range(UNITS)]
    for g in range(UNITS):
        steps += [(g + STAGGER * i, g, i) for i in range(1, 2 * bits + 1)]
        steps.append((g + STAGGER * 2 * bits + 0.5, g, 2 * bits + 1))
    return orders, [(g, i) for _, g, i in sorted(steps)]


def permuted(index, order):
    bits = len(order)
    return sum(((index // 2**b) % 2) * 2 ** (bits - 1 - at) for at, b in enumerate(order))


def twiddles(no, lon_local, orders):
    blocks = -(-lon_local // LANES)
    period = no * lon_local

    def turn(positions):
        phase = np.outer(positions, np.arange(orders)) % period
        angle = phase * (2.0 * math.pi / period)
        return np.cos(angle), np.sin(angle)

    fine = np.concatenate(turn(np.arange(LANES)), 1)
    high = fine.astype(BF16)
    low = (fine - high.astype(np.float64)).astype(BF16)
    starts = (lon_local * np.arange(no)[:, None] + LANES * np.arange(blocks)).reshape(-1)
    cos, sin = turn(starts)
    return np.concatenate([high, low], 0), cos.astype(np.float32), sin.astype(np.float32)


def kernel(
    n, no,
    press_hbm, tables_ref, quad_hbm, love_hbm, order_hbm, cycle_hbm, fine_hbm, cos_hbm, sin_hbm,
    spec_hbm, field_hbm,
    tab, press_ref, quad_ref, love_ref, order_ref, cycle_ref, fine, cos_q, sin_q,
    gathered, wide, partial, orders_ref, pick, lhs, part, landed, scaled,
    spec_ref, field_ref, signals, rotated, out_signal, in_signal,
    tab_sem, in_sem, spec_sem, press_sem, send_sem, hop_sem, field_sem,
):
    bits = n.bit_length() - 1
    me = lax.axis_index("lat")
    core = lax.axis_index("ord")
    orders_of, steps = plan(bits)
    groups = len(orders_of)
    per_unit = groups // UNITS
    cycles = press_ref.shape[1]
    lon_local = press_ref.shape[2]
    local_orders = orders_ref.shape[0]
    degrees = tables_ref.shape[1]
    share = degrees // n
    go = local_orders // groups
    rows_g = go * cycles
    uo = local_orders // UNITS
    rows_u = uo * cycles
    both = 2 * cycles
    blocks = max(1, min(n, 1024 // share))
    width = blocks * share
    period = lon_local * no
    turns = cos_q.shape[0] // no
    modes = order_ref.shape[1]

    barrier = pltpu.get_barrier_semaphore()
    partners = []
    for b in range(bits):
        mine = (me // 2**b) % 2
        partners.append(me + (1 - 2 * mine) * 2**b)
    peers = [lax.rem(core + i, no) for i in range(1, no)]
    for peer in peers:
        pl.semaphore_signal(barrier, inc=1, device_id=(me, peer), device_id_type=MESH)
    for partner in partners:
        pl.semaphore_signal(barrier, inc=1, device_id=(partner, core), device_id_type=MESH)

    loads = []
    pairs = (
        (press_hbm, press_ref), (order_hbm, order_ref), (quad_hbm, quad_ref), (cycle_hbm, cycle_ref),
        (fine_hbm, fine), (cos_hbm, cos_q), (sin_hbm, sin_q), (love_hbm, love_ref),
    )
    for i, (source, to) in enumerate(pairs):
        copy = pltpu.make_async_copy(source, to, in_sem.at[i])
        copy.start()
        loads.append(copy)
    loads[0].wait()
    pl.semaphore_wait(barrier, bits + no - 1)
    press_copies = []
    for i, peer in enumerate(peers):
        copy = pltpu.make_async_remote_copy(
            src_ref=press_ref,
            dst_ref=gathered.at[i],
            send_sem=press_sem.at[0, i],
            recv_sem=press_sem.at[1, i],
            device_id=(me, peer),
            device_id_type=MESH,
        )
        copy.start()
        press_copies.append(copy)

    def widen(at, piece):
        for q in range(turns):
            first = q * LANES
            count = min(LANES, lon_local - first)
            rows = jnp.concatenate([piece[h, :, first : first + count].astype(F32) for h in range(2)], 0)
            if count < LANES:
                rows = jnp.concatenate([rows, jnp.zeros((both, LANES - count), F32)], 1)
            rows = rows.astype(BF16)
            wide[at, q * both : (q + 1) * both, :LANES] = rows
            wide[at, q * both : (q + 1) * both, LANES:] = rows

    def transform(at, origin, start):
        partial[...] = jnp.dot(wide[at], fine[...], preferred_element_type=F32)

        cos_sum, sin_sum = start
        for q in range(turns):
            rows = slice(q * both, (q + 1) * both)
            c = partial[rows, :modes]
            s = partial[rows, modes:]
            cq = cos_q[pl.ds(origin * turns + q, 1), :]
            sq = sin_q[pl.ds(origin * turns + q, 1), :]
            cos_sum = cos_sum + (cq * c - sq * s)
            sin_sum = sin_sum + (sq * c + cq * s)
        return cos_sum, sin_sum

    widen(0, press_ref)
    for copy in loads[1:]:
        copy.wait()
    tab_copies = {}
    for u in [g // per_unit for g, i in steps if i == 0]:
        rows = pl.ds(u * rows_u, rows_u)
        copy = pltpu.make_async_copy(tables_ref.at[rows], tab.at[rows], tab_sem.at[u])
        copy.start()
        tab_copies[u] = copy
    shape = (local_orders, modes)
    slot = core * local_orders + lax.broadcasted_iota(jnp.int32, shape, 0)
    lane = lax.broadcasted_iota(jnp.int32, shape, 1)
    order_col = jnp.sum(
        jnp.where(slot == lane, order_ref[...].astype(F32), 0.0), axis=1, keepdims=True
    ).astype(jnp.int32)
    orders_ref[...] = order_col
    pick[...] = jnp.where(order_col == lane, 1.0, 0.0).astype(BF16)

    square = (cycles, cycles)
    eye = lax.broadcasted_iota(jnp.int32, square, 0) == lax.broadcasted_iota(jnp.int32, square, 1)
    cycle_col = jnp.sum(
        jnp.where(eye, cycle_ref[...].astype(F32), 0.0), axis=1, keepdims=True
    ).astype(jnp.int32)
    quad_lane = lax.broadcasted_iota(jnp.int32, (cycles, quad_ref.shape[1]), 1)
    weight = jnp.sum(jnp.where(quad_lane == cycle_col, quad_ref[...], 0.0), axis=1, keepdims=True)
    weight = weight * (1.0 / math.sqrt(quad_ref.shape[1])) * (1.0 / math.sqrt(period))

    col = lax.broadcasted_iota(jnp.int32, (uo, rows_u), 1) // cycles
    row = lax.broadcasted_iota(jnp.int32, (uo, rows_u), 0)
    diagonal = row == col
    spread_row = lax.broadcasted_iota(jnp.int32, (4 * cycles, 4 * rows_u), 0)
    spread_col = lax.broadcasted_iota(jnp.int32, (4 * cycles, 4 * rows_u), 1)
    spread = jnp.where(
        spread_row == (spread_col // rows_u) * cycles + spread_col % cycles, 1.0, 0.0
    ).astype(BF16)
    lane_order = lax.broadcasted_iota(jnp.int32, (cycles, 4 * go), 1) % go

    zero = jnp.zeros((both, modes), F32)
    sums = transform(0, core, (zero, zero))
    for i, copy in enumerate(press_copies):
        copy.wait()
        widen(i + 1, gathered.at[i])
        sums = transform(i + 1, lax.rem(core + no - 1 - i, no), sums)
    cos_sum, sin_sum = sums
    folded = jnp.concatenate(
        [
            weight * (cos_sum[:cycles] + cos_sum[cycles:]),
            -weight * (sin_sum[:cycles] + sin_sum[cycles:]),
            weight * (cos_sum[:cycles] - cos_sum[cycles:]),
            -weight * (sin_sum[:cycles] - sin_sum[cycles:]),
        ],
        0,
    ).astype(BF16)
    chosen = lax.dot_general(pick[...], folded, NT, preferred_element_type=F32).astype(BF16)
    repeated = jnp.dot(chosen, spread, preferred_element_type=F32)
    for u in range(UNITS):
        rows = repeated[u * uo : (u + 1) * uo]
        lhs[u] = jnp.concatenate(
            [jnp.where(diagonal, rows[:, c * rows_u : (c + 1) * rows_u], 0.0) for c in range(4)], 0
        ).astype(BF16)

    def parity(start, count, first):
        degree = first + lax.broadcasted_iota(jnp.int32, (count, width), 1)
        order = orders_ref[start : start + count, :]
        return (degree + order) & 1 == 0, degree >= order

    def region(g, k):
        base = 0
        for at in range(k):
            base = base + ((me // 2 ** orders_of[g][at]) % 2) * (n >> (at + 1))
        return base

    def analyse(u):
        tab_copies[u].wait()
        left = lhs[u]
        for i in range(degrees // width):
            first = i * width
            product = jnp.dot(
                left, tab[u * rows_u : (u + 1) * rows_u, first : first + width],
                preferred_element_type=F32,
            )
            even, present = parity(u * uo, uo, first)
            real = jnp.where(present, jnp.where(even, product[:uo], product[2 * uo : 3 * uo]), 0.0)
            imag = jnp.where(present, jnp.where(even, product[uo : 2 * uo], product[3 * uo :]), 0.0)
            for v in range(per_unit):
                g = u * per_unit + v
                rows = slice(v * go, (v + 1) * go)
                value = jnp.concatenate([real[rows], imag[rows]], 0).astype(BF16)
                for j in range(blocks):
                    to = permuted(i * blocks + j, orders_of[g])
                    part[g, to] = value[:, j * share : (j + 1) * share]

    reduce_copies = {}
    gather_copies = {}

    def send_reduce(g, k):
        h = n >> (k + 1)
        b = orders_of[g][k]
        mine = (me // 2**b) % 2
        copy = pltpu.make_async_remote_copy(
            src_ref=part.at[g, pl.ds(region(g, k) + (1 - mine) * h, h)],
            dst_ref=landed.at[g, pl.ds(n - (n >> k), h)],
            send_sem=send_sem.at[0],
            recv_sem=hop_sem.at[g, k],
            device_id=(partners[b], core),
            device_id_type=MESH,
        )
        copy.start()
        reduce_copies[g, k] = copy

    def take_reduce(g, k):
        h = n >> (k + 1)
        reduce_copies[g, k].wait_recv()
        keep = region(g, k + 1)
        off = n - (n >> k)
        if k < bits - 1:

            def add(i, carry):
                part[g, keep + i] = (
                    part[g, keep + i].astype(F32) + landed[g, off + i].astype(F32)
                ).astype(BF16)
                return carry

            lax.fori_loop(0, h, add, 0, unroll=min(h, 4))
            send_reduce(g, k + 1)
            return
        total = part[g, keep].astype(F32) + landed[g, off].astype(F32)
        spec_ref[0, g * go : (g + 1) * go, :] = total[:go]
        spec_ref[1, g * go : (g + 1) * go, :] = total[go:]
        scaled[g, keep] = (DENSITY_RATIO * (1.0 + love_ref[pl.ds(me, 1), :]) * total).astype(BF16)
        send_gather(g, bits - 1)

    def send_gather(g, k):
        h = n >> (k + 1)
        b = orders_of[g][k]
        mine = pl.ds(region(g, k + 1), h)
        copy = pltpu.make_async_remote_copy(
            src_ref=scaled.at[g, mine],
            dst_ref=scaled.at[g, mine],
            send_sem=send_sem.at[1],
            recv_sem=hop_sem.at[g, (k - 1) % (bits + 1)],
            device_id=(partners[b], core),
            device_id_type=MESH,
        )
        copy.start()
        gather_copies[g, k] = copy

    def take_gather(g, k):
        gather_copies[g, k].wait_recv()
        if k > 0:
            send_gather(g, k - 1)

    def synthesise(g):
        signal = jnp.zeros((cycles, 4 * go), F32)
        for i in range(degrees // width):
            first = i * width
            even, _ = parity(g * go, go, first)
            pieces = [scaled[g, permuted(i * blocks + j, orders_of[g])] for j in range(blocks)]
            both_parts = jnp.concatenate(pieces, 1).astype(F32)
            real, imag = both_parts[:go], both_parts[go:]
            stacked = jnp.concatenate(
                [real, imag, jnp.where(even, real, -real), jnp.where(even, imag, -imag)], 0
            ).astype(BF16)
            total = lax.dot_general(
                tab[g * rows_g : (g + 1) * rows_g, first : first + width], stacked, NT,
                preferred_element_type=F32,
            )
            piece = jnp.zeros((cycles, 4 * go), F32)
            for o in range(go):
                piece = jnp.where(lane_order == o, total[o * cycles : (o + 1) * cycles], piece)
            signal = signal + piece
        signal = signal * (1.0 / math.sqrt(degrees))
        for c in range(4):
            signals[c * cycles : (c + 1) * cycles, g * go : (g + 1) * go] = signal[:, c * go : (c + 1) * go]

    spec_copy = pltpu.make_async_copy(spec_ref, spec_hbm, spec_sem.at[0])
    last_sum = max(at for at, (_, i) in enumerate(steps) if i == bits)
    for at, (g, i) in enumerate(steps):
        if at == last_sum + 1:
            spec_copy.start()
        if i == 0:
            analyse(g // per_unit)
            for v in range(per_unit):
                send_reduce(g + v, 0)
        elif i <= bits:
            take_reduce(g, i - 1)
        elif i <= 2 * bits:
            take_gather(g, 2 * bits - i)
        else:
            synthesise(g)

    natural = jnp.dot(signals[...].astype(BF16), pick[...], preferred_element_type=F32)
    out_signal[...] = natural.astype(BF16)
    field_copies = []
    for i, peer in enumerate(peers):
        copy = pltpu.make_async_remote_copy(
            src_ref=out_signal,
            dst_ref=in_signal.at[i],
            send_sem=field_sem.at[0, i],
            recv_sem=field_sem.at[1, i],
            device_id=(me, peer),
            device_id_type=MESH,
        )
        copy.start()
        field_copies.append(copy)
    total = natural
    for i, copy in enumerate(field_copies):
        copy.wait_recv()
        total = total + in_signal[i].astype(F32)
    total = total * (1.0 / math.sqrt(modes))
    real = jnp.concatenate([total[:cycles], total[2 * cycles : 3 * cycles]], 0)
    imag = jnp.concatenate([total[cycles : 2 * cycles], total[3 * cycles :]], 0)
    for q in range(turns):
        cq = cos_q[pl.ds(core * turns + q, 1), :]
        sq = sin_q[pl.ds(core * turns + q, 1), :]
        rows = slice(q * both, (q + 1) * both)
        rotated[rows, :modes] = (real * cq - imag * sq).astype(BF16)
        rotated[rows, modes:] = (-real * sq - imag * cq).astype(BF16)
    parts = lax.dot_general(rotated[...], fine[...], NT, preferred_element_type=F32)
    field = parts[:, :LANES] + parts[:, LANES:]
    for q in range(turns):
        first = q * LANES
        count = min(LANES, lon_local - first)
        for h in range(2):
            at = q * both + h * cycles
            field_ref[h, :, first : first + count] = field[at : at + cycles, :count]
    field_copy = pltpu.make_async_copy(field_ref, field_hbm, spec_sem.at[1])
    field_copy.start()
    for i, blocks_ref in enumerate((part, scaled)):
        sent = blocks_ref.at[:, pl.ds(0, n - 1)]
        pltpu.make_async_copy(sent, sent, send_sem.at[i]).wait()
    for copy in field_copies:
        copy.wait_send()
    spec_copy.wait()
    field_copy.wait()


def finish(half_spec, half_field, spec_ref, field_ref):
    spec_ref[...] = half_spec[...]
    field_ref[...] = half_field[...]


def per_device(n, no, pressure, tables, quad_weight, love_number, order_list, cycle_list):
    _, cycles, lon_local = pressure.shape
    local_orders, _, degrees = tables.shape
    bits = n.bit_length() - 1
    share = degrees // n
    groups = len(plan(bits)[0])
    go = local_orders // groups
    uo = local_orders // UNITS
    modes = order_list.shape[0]
    turns = -(-lon_local // LANES)
    fine, cos_q, sin_q = [jnp.asarray(table) for table in twiddles(no, lon_local, modes)]
    small = (
        quad_weight[None, :], love_number.reshape(n, share), order_list[None, :], cycle_list[None, :],
        fine, cos_q, sin_q,
    )
    vmem = pl.BlockSpec(memory_space=pltpu.VMEM)
    hbm = pl.BlockSpec(memory_space=pl.ANY)
    blocks = pltpu.VMEM((groups, n, 2 * go, share), BF16)
    spectrum, field = pl.pallas_call(
        functools.partial(kernel, n, no),
        out_shape=(
            jax.ShapeDtypeStruct((2, local_orders, share), F32),
            jax.ShapeDtypeStruct((2, cycles, lon_local), F32),
        ),
        in_specs=[hbm] * 9,
        out_specs=(hbm, hbm),
        scratch_shapes=[
            pltpu.VMEM((local_orders * cycles, degrees), BF16),
            pltpu.VMEM((2, cycles, lon_local), BF16),
            *[pltpu.VMEM(array.shape, array.dtype) for array in small],
            pltpu.VMEM((no - 1, 2, cycles, lon_local), BF16),
            pltpu.VMEM((no, turns * 2 * cycles, 2 * LANES), BF16),
            pltpu.VMEM((turns * 2 * cycles, 2 * modes), F32),
            pltpu.VMEM((local_orders, 1), jnp.int32),
            pltpu.VMEM((local_orders, modes), BF16),
            pltpu.VMEM((UNITS, 4 * uo, uo * cycles), BF16),
            blocks, blocks, blocks,
            pltpu.VMEM((2, local_orders, share), F32),
            pltpu.VMEM((2, cycles, lon_local), F32),
            pltpu.VMEM((4 * cycles, local_orders), F32),
            pltpu.VMEM((turns * 2 * cycles, 2 * modes), BF16),
            pltpu.VMEM((4 * cycles, modes), BF16),
            pltpu.VMEM((no - 1, 4 * cycles, modes), BF16),
            pltpu.SemaphoreType.DMA((UNITS,)),
            pltpu.SemaphoreType.DMA((8,)),
            pltpu.SemaphoreType.DMA((2,)),
            pltpu.SemaphoreType.DMA((2, no - 1)),
            pltpu.SemaphoreType.DMA((2,)),
            pltpu.SemaphoreType.DMA((groups, bits + 1)),
            pltpu.SemaphoreType.DMA((2, no - 1)),
        ],
        compiler_params=pltpu.CompilerParams(
            collective_id=0, has_side_effects=True, vmem_limit_bytes=56 * 1024 * 1024
        ),
    )(pressure, tables.reshape(local_orders * cycles, degrees), *small)
    return pl.pallas_call(
        finish,
        out_shape=(
            jax.ShapeDtypeStruct(spectrum.shape, F32),
            jax.ShapeDtypeStruct(field.shape, F32),
        ),
        in_specs=[vmem, vmem],
        out_specs=(vmem, vmem),
    )(spectrum, field)


def solution(mesh):
    placed = (P(None, "lat", "ord"), P("ord", "lat", None), P(), P(), P(), P("lat"))
    return jax.shard_map(
        functools.partial(per_device, mesh.shape["lat"], mesh.shape["ord"]),
        mesh=mesh,
        in_specs=placed,
        out_specs=(P(None, "ord", "lat"), P(None, "lat", "ord")),
        check_vma=False,
    )
```

```python
import functools
import math

import jax
import jax.numpy as jnp
import numpy as np
from jax import lax
from jax.experimental import pallas as pl
from jax.experimental.pallas import tpu as pltpu
from jax.sharding import PartitionSpec as P

DENSITY_RATIO = 3.0 * 1025.0 / 5517.0
LANES = 128
UNITS = 8
STAGGER = 4
MESH = pl.DeviceIdType.MESH
NT = (((1,), (1,)), ((), ()))
F32 = jnp.float32
BF16 = jnp.bfloat16


PLAN_ORDERS = (
    (1, 3, 0, 2), (2, 1, 0, 3), (2, 0, 1, 3), (0, 1, 2, 3), (1, 0, 2, 3), (0, 1, 3, 2),
    (1, 0, 2, 3), (2, 3, 1, 0), (0, 2, 1, 3), (0, 1, 2, 3), (2, 0, 1, 3), (1, 0, 3, 2),
    (2, 0, 1, 3), (1, 2, 0, 3), (0, 1, 2, 3), (2, 1, 0, 3),
)
PLAN_STEPS = (
    160, 64, 96, 128, 0, 161, 81, 32, 113, 224, 145, 129, 162, 97, 17, 1, 177, 33, 192, 225, 163,
    65, 241, 146, 18, 82, 130, 98, 178, 49, 209, 2, 34, 114, 226, 193, 66, 164, 19, 242, 147, 99,
    83, 131, 35, 115, 179, 3, 50, 210, 227, 67, 243, 194, 84, 148, 165, 100, 20, 211, 36, 4, 116,
    180, 195, 228, 132, 68, 244, 51, 166, 149, 101, 21, 85, 5, 37, 181, 117, 196, 212, 133, 69, 229,
    245, 150, 52, 6, 22, 102, 86, 38, 167, 134, 197, 246, 213, 182, 230, 151, 70, 53, 103, 87, 118,
    198, 7, 247, 135, 54, 214, 183, 168, 169, 39, 23, 231, 152, 153, 71, 104, 105, 119, 88, 89, 199,
    8, 9, 248, 55, 249, 136, 215, 137, 184, 185, 232, 40, 233, 41, 72, 24, 25, 73, 120, 121, 200,
    201, 56, 57, 216, 217,
)


def plan(bits):
    if bits == len(PLAN_ORDERS[0]):
        return [list(order) for order in PLAN_ORDERS], [divmod(code, 16) for code in PLAN_STEPS]
    base = list(range(bits))
    orders = [base]
    if bits >= 3:
        a, b, c, d, e, f = [
            list(head) + base[3:]
            for head in ((0, 1, 2), (1, 0, 2), (2, 0, 1), (2, 1, 0), (0, 2, 1), (1, 2, 0))
        ]
        orders = [a, b, c, e, f, d, a, b]
    orders = [orders[g % len(orders)] for g in range(UNITS)]
    steps = [(g - UNITS, g, 0) for g in range(UNITS)]
    for g in range(UNITS):
        steps += [(g + STAGGER * i, g, i) for i in range(1, 2 * bits + 1)]
        steps.append((g + STAGGER * 2 * bits + 0.5, g, 2 * bits + 1))
    return orders, [(g, i) for _, g, i in sorted(steps)]


def shared_slots(bits, orders, steps):
    per_unit = len(orders) // UNITS
    take, send = {}, {}
    for at, (g, i) in enumerate(steps):
        if i == 0:
            send.update({(g + v, 0): at for v in range(per_unit)})
        elif i <= 2 * bits:
            take[g, i - 1] = at
            send[g, i] = at

    def along(message):
        g, hop = message
        return orders[g][min(hop, 2 * bits - 1 - hop)]

    free_after, slots = [], {}
    for message in sorted(take, key=lambda m: (send[m], m)):
        known = max(
            (send[m] for m in take if along(m) == along(message) and take[m] <= send[message]),
            default=-1,
        )
        fits = [s for s, at in enumerate(free_after) if at <= known]
        slot = max(fits, key=lambda s: free_after[s]) if fits else len(free_after)
        if not fits:
            free_after.append(0)
        free_after[slot] = take[message]
        slots[message] = slot
    return slots


def permuted(index, order):
    bits = len(order)
    return sum(((index // 2**b) % 2) * 2 ** (bits - 1 - at) for at, b in enumerate(order))


def twiddles(no, lon_local, orders):
    blocks = -(-lon_local // LANES)
    period = no * lon_local

    def turn(positions):
        phase = np.outer(positions, np.arange(orders)) % period
        angle = phase * (2.0 * math.pi / period)
        return np.cos(angle), np.sin(angle)

    fine = np.concatenate(turn(np.arange(LANES)), 1)
    high = fine.astype(BF16)
    low = (fine - high.astype(np.float64)).astype(BF16)
    starts = (lon_local * np.arange(no)[:, None] + LANES * np.arange(blocks)).reshape(-1)
    cos, sin = turn(starts)
    fine = np.concatenate([high, low], 0)
    return fine, cos.astype(np.float32), sin.astype(np.float32), np.ascontiguousarray(fine.T)


def kernel(
    n, no,
    press_hbm, tables_ref, quad_hbm, love_hbm, order_hbm, cycle_hbm, fine_hbm, cos_hbm, sin_hbm, back_hbm,
    spec_hbm, field_hbm,
    tab, press_ref, quad_ref, love_ref, order_ref, cycle_ref, fine, cos_q, sin_q, back,
    gathered, wide, partial, orders_ref, pick, repeated, part, landed, scaled,
    spec_ref, field_ref, signals, rotated, out_signal, in_signal,
    tab_sem, in_sem, spec_sem, press_sem, send_sem, hop_sem, field_sem,
):
    bits = n.bit_length() - 1
    me = lax.axis_index("lat")
    core = lax.axis_index("ord")
    orders_of, steps = plan(bits)
    slots = shared_slots(bits, orders_of, steps)
    groups = len(orders_of)
    per_unit = groups // UNITS
    cycles = press_ref.shape[1]
    lon_local = press_ref.shape[2]
    local_orders = orders_ref.shape[0]
    degrees = tables_ref.shape[1]
    share = degrees // n
    go = local_orders // groups
    rows_g = go * cycles
    uo = local_orders // UNITS
    rows_u = uo * cycles
    both = 2 * cycles
    blocks = max(1, min(n, 1024 // share))
    width = blocks * share
    period = lon_local * no
    turns = cos_q.shape[0] // no
    modes = order_ref.shape[1]

    barrier = pltpu.get_barrier_semaphore()
    partners = []
    for b in range(bits):
        mine = (me // 2**b) % 2
        partners.append(me + (1 - 2 * mine) * 2**b)
    peers = [lax.rem(core + i, no) for i in range(1, no)]
    for peer in peers:
        pl.semaphore_signal(barrier, inc=1, device_id=(me, peer), device_id_type=MESH)
    for partner in partners:
        pl.semaphore_signal(barrier, inc=1, device_id=(partner, core), device_id_type=MESH)

    loads = []
    pairs = (
        (press_hbm, press_ref), (order_hbm, order_ref), (quad_hbm, quad_ref), (cycle_hbm, cycle_ref),
        (fine_hbm, fine), (cos_hbm, cos_q), (sin_hbm, sin_q), (love_hbm, love_ref),
    )
    for i, (source, to) in enumerate(pairs):
        copy = pltpu.make_async_copy(source, to, in_sem.at[i])
        copy.start()
        loads.append(copy)
    loads[0].wait()
    pl.semaphore_wait(barrier, bits + no - 1)
    press_copies = []
    for i, peer in enumerate(peers):
        copy = pltpu.make_async_remote_copy(
            src_ref=press_ref,
            dst_ref=gathered.at[i],
            send_sem=press_sem.at[0, i],
            recv_sem=press_sem.at[1, i],
            device_id=(me, peer),
            device_id_type=MESH,
        )
        copy.start()
        press_copies.append(copy)

    def widen(at, piece):
        for q in range(turns):
            first = q * LANES
            count = min(LANES, lon_local - first)
            rows = jnp.concatenate([piece[h, :, first : first + count].astype(F32) for h in range(2)], 0)
            if count < LANES:
                rows = jnp.concatenate([rows, jnp.zeros((both, LANES - count), F32)], 1)
            rows = rows.astype(BF16)
            wide[at, q * both : (q + 1) * both, :LANES] = rows
            wide[at, q * both : (q + 1) * both, LANES:] = rows

    def transform(at, origin, start):
        partial[...] = jnp.dot(wide[at], fine[...], preferred_element_type=F32)

        cos_sum, sin_sum = start
        for q in range(turns):
            rows = slice(q * both, (q + 1) * both)
            c = partial[rows, :modes]
            s = partial[rows, modes:]
            cq = cos_q[pl.ds(origin * turns + q, 1), :]
            sq = sin_q[pl.ds(origin * turns + q, 1), :]
            cos_sum = cos_sum + (cq * c - sq * s)
            sin_sum = sin_sum + (sq * c + cq * s)
        return cos_sum, sin_sum

    widen(0, press_ref)
    for copy in loads[1:]:
        copy.wait()
    tab_copies = {}
    for u in [g // per_unit for g, i in steps if i == 0]:
        rows = pl.ds(u * rows_u, rows_u)
        copy = pltpu.make_async_copy(tables_ref.at[rows], tab.at[rows], tab_sem.at[u])
        copy.start()
        tab_copies[u] = copy
    back_copy = pltpu.make_async_copy(back_hbm, back, in_sem.at[8])
    back_copy.start()
    shape = (local_orders, modes)
    slot = core * local_orders + lax.broadcasted_iota(jnp.int32, shape, 0)
    lane = lax.broadcasted_iota(jnp.int32, shape, 1)
    order_col = jnp.sum(
        jnp.where(slot == lane, order_ref[...].astype(F32), 0.0), axis=1, keepdims=True
    ).astype(jnp.int32)
    orders_ref[...] = order_col
    pick[...] = jnp.where(order_col == lane, 1.0, 0.0).astype(BF16)

    square = (cycles, cycles)
    eye = lax.broadcasted_iota(jnp.int32, square, 0) == lax.broadcasted_iota(jnp.int32, square, 1)
    cycle_col = jnp.sum(
        jnp.where(eye, cycle_ref[...].astype(F32), 0.0), axis=1, keepdims=True
    ).astype(jnp.int32)
    quad_lane = lax.broadcasted_iota(jnp.int32, (cycles, quad_ref.shape[1]), 1)
    weight = jnp.sum(jnp.where(quad_lane == cycle_col, quad_ref[...], 0.0), axis=1, keepdims=True)
    weight = weight * (1.0 / math.sqrt(quad_ref.shape[1])) * (1.0 / math.sqrt(period))

    col = lax.broadcasted_iota(jnp.int32, (uo, rows_u), 1) // cycles
    row = lax.broadcasted_iota(jnp.int32, (uo, rows_u), 0)
    diagonal = row == col
    spread_row = lax.broadcasted_iota(jnp.int32, (4 * cycles, 4 * rows_u), 0)
    spread_col = lax.broadcasted_iota(jnp.int32, (4 * cycles, 4 * rows_u), 1)
    spread = jnp.where(
        spread_row == (spread_col // rows_u) * cycles + spread_col % cycles, 1.0, 0.0
    ).astype(BF16)
    lane_order = lax.broadcasted_iota(jnp.int32, (cycles, 4 * go), 1) % go

    zero = jnp.zeros((both, modes), F32)
    sums = transform(0, core, (zero, zero))
    for i, copy in enumerate(press_copies):
        copy.wait()
        widen(i + 1, gathered.at[i])
        sums = transform(i + 1, lax.rem(core + no - 1 - i, no), sums)
    cos_sum, sin_sum = sums
    folded = jnp.concatenate(
        [
            weight * (cos_sum[:cycles] + cos_sum[cycles:]),
            -weight * (sin_sum[:cycles] + sin_sum[cycles:]),
            weight * (cos_sum[:cycles] - cos_sum[cycles:]),
            -weight * (sin_sum[:cycles] - sin_sum[cycles:]),
        ],
        0,
    ).astype(BF16)
    chosen = lax.dot_general(pick[...], folded, NT, preferred_element_type=F32).astype(BF16)
    repeated[...] = jnp.dot(chosen, spread, preferred_element_type=F32)
    def parity(start, count, first):
        degree = first + lax.broadcasted_iota(jnp.int32, (count, width), 1)
        order = orders_ref[start : start + count, :]
        return (degree + order) & 1 == 0, degree >= order

    def region(g, k):
        base = 0
        for at in range(k):
            base = base + ((me // 2 ** orders_of[g][at]) % 2) * (n >> (at + 1))
        return base

    def analyse(u):
        tab_copies[u].wait()
        rows = repeated[u * uo : (u + 1) * uo, :]
        left = jnp.concatenate(
            [jnp.where(diagonal, rows[:, c * rows_u : (c + 1) * rows_u], 0.0) for c in range(4)], 0
        ).astype(BF16)
        for i in range(degrees // width):
            first = i * width
            product = jnp.dot(
                left, tab[u * rows_u : (u + 1) * rows_u, first : first + width],
                preferred_element_type=F32,
            )
            even, present = parity(u * uo, uo, first)
            real = jnp.where(present, jnp.where(even, product[:uo], product[2 * uo : 3 * uo]), 0.0)
            imag = jnp.where(present, jnp.where(even, product[uo : 2 * uo], product[3 * uo :]), 0.0)
            for v in range(per_unit):
                g = u * per_unit + v
                rows = slice(v * go, (v + 1) * go)
                value = jnp.concatenate([real[rows], imag[rows]], 0).astype(BF16)
                for j in range(blocks):
                    to = permuted(i * blocks + j, orders_of[g])
                    part[g, to] = value[:, j * share : (j + 1) * share]

    reduce_copies = {}
    gather_copies = {}

    def send_reduce(g, k):
        h = n >> (k + 1)
        b = orders_of[g][k]
        mine = (me // 2**b) % 2
        copy = pltpu.make_async_remote_copy(
            src_ref=part.at[g, pl.ds(region(g, k) + (1 - mine) * h, h)],
            dst_ref=landed.at[g, pl.ds(n - (n >> k), h)],
            send_sem=send_sem.at[0],
            recv_sem=hop_sem.at[slots[g, k]],
            device_id=(partners[b], core),
            device_id_type=MESH,
        )
        copy.start()
        reduce_copies[g, k] = copy

    def take_reduce(g, k):
        h = n >> (k + 1)
        reduce_copies[g, k].wait_recv()
        keep = region(g, k + 1)
        off = n - (n >> k)
        if k < bits - 1:

            def add(i, carry):
                part[g, keep + i] = (
                    part[g, keep + i].astype(F32) + landed[g, off + i].astype(F32)
                ).astype(BF16)
                return carry

            lax.fori_loop(0, h, add, 0, unroll=min(h, 4))
            send_reduce(g, k + 1)
            return
        total = part[g, keep].astype(F32) + landed[g, off].astype(F32)
        spec_ref[0, g * go : (g + 1) * go, :] = total[:go]
        spec_ref[1, g * go : (g + 1) * go, :] = total[go:]
        scaled[g, keep] = (DENSITY_RATIO * (1.0 + love_ref[pl.ds(me, 1), :]) * total).astype(BF16)
        send_gather(g, bits - 1)

    def send_gather(g, k):
        h = n >> (k + 1)
        b = orders_of[g][k]
        mine = pl.ds(region(g, k + 1), h)
        copy = pltpu.make_async_remote_copy(
            src_ref=scaled.at[g, mine],
            dst_ref=scaled.at[g, mine],
            send_sem=send_sem.at[1],
            recv_sem=hop_sem.at[slots[g, 2 * bits - 1 - k]],
            device_id=(partners[b], core),
            device_id_type=MESH,
        )
        copy.start()
        gather_copies[g, k] = copy

    def take_gather(g, k):
        gather_copies[g, k].wait_recv()
        if k > 0:
            send_gather(g, k - 1)

    def synthesise(g):
        signal = jnp.zeros((cycles, 4 * go), F32)
        for i in range(degrees // width):
            first = i * width
            even, _ = parity(g * go, go, first)
            pieces = [scaled[g, permuted(i * blocks + j, orders_of[g])] for j in range(blocks)]
            both_parts = jnp.concatenate(pieces, 1).astype(F32)
            real, imag = both_parts[:go], both_parts[go:]
            stacked = jnp.concatenate(
                [real, imag, jnp.where(even, real, -real), jnp.where(even, imag, -imag)], 0
            ).astype(BF16)
            total = lax.dot_general(
                tab[g * rows_g : (g + 1) * rows_g, first : first + width], stacked, NT,
                preferred_element_type=F32,
            )
            piece = jnp.zeros((cycles, 4 * go), F32)
            for o in range(go):
                piece = jnp.where(lane_order == o, total[o * cycles : (o + 1) * cycles], piece)
            signal = signal + piece
        signal = signal * (1.0 / math.sqrt(degrees))
        for c in range(4):
            signals[c * cycles : (c + 1) * cycles, g * go : (g + 1) * go] = signal[:, c * go : (c + 1) * go]

    spec_copy = pltpu.make_async_copy(spec_ref, spec_hbm, spec_sem.at[0])
    last_sum = max(at for at, (_, i) in enumerate(steps) if i == bits)
    for at, (g, i) in enumerate(steps):
        if at == last_sum + 1:
            spec_copy.start()
        if i == 0:
            analyse(g // per_unit)
            for v in range(per_unit):
                send_reduce(g + v, 0)
        elif i <= bits:
            take_reduce(g, i - 1)
        elif i <= 2 * bits:
            take_gather(g, 2 * bits - i)
        else:
            synthesise(g)

    back_copy.wait()
    natural = jnp.dot(signals[...].astype(BF16), pick[...], preferred_element_type=F32)
    out_signal[...] = natural.astype(BF16)
    field_copies = []
    for i, peer in enumerate(peers):
        copy = pltpu.make_async_remote_copy(
            src_ref=out_signal,
            dst_ref=in_signal.at[i],
            send_sem=field_sem.at[0, i],
            recv_sem=field_sem.at[1, i],
            device_id=(me, peer),
            device_id_type=MESH,
        )
        copy.start()
        field_copies.append(copy)
    total = natural
    for i, copy in enumerate(field_copies):
        copy.wait_recv()
        total = total + in_signal[i].astype(F32)
    total = total * (1.0 / math.sqrt(modes))
    real = jnp.concatenate([total[:cycles], total[2 * cycles : 3 * cycles]], 0)
    imag = jnp.concatenate([total[cycles : 2 * cycles], total[3 * cycles :]], 0)
    for q in range(turns):
        cq = cos_q[pl.ds(core * turns + q, 1), :]
        sq = sin_q[pl.ds(core * turns + q, 1), :]
        rows = slice(q * both, (q + 1) * both)
        rotated[rows, :modes] = (real * cq - imag * sq).astype(BF16)
        rotated[rows, modes:] = (-real * sq - imag * cq).astype(BF16)
    parts = jnp.dot(rotated[...], back[...], preferred_element_type=F32)
    field = parts[:, :LANES] + parts[:, LANES:]
    for q in range(turns):
        first = q * LANES
        count = min(LANES, lon_local - first)
        for h in range(2):
            at = q * both + h * cycles
            field_ref[h, :, first : first + count] = field[at : at + cycles, :count]
    field_copy = pltpu.make_async_copy(field_ref, field_hbm, spec_sem.at[1])
    field_copy.start()
    for i, blocks_ref in enumerate((part, scaled)):
        sent = blocks_ref.at[:, pl.ds(0, n - 1)]
        pltpu.make_async_copy(sent, sent, send_sem.at[i]).wait()
    for copy in field_copies:
        copy.wait_send()
    spec_copy.wait()
    field_copy.wait()


def finish(half_spec, half_field, spec_ref, field_ref, spec, field, sems):
    pairs = ((half_spec, spec, spec_ref), (half_field, field, field_ref))
    loads = [pltpu.make_async_copy(a, b, sems.at[0, i]) for i, (a, b, _) in enumerate(pairs)]
    stores = [pltpu.make_async_copy(b, c, sems.at[1, i]) for i, (_, b, c) in enumerate(pairs)]
    for load in loads:
        load.start()
    for load, store in zip(loads, stores):
        load.wait()
        store.start()
    for store in stores:
        store.wait()


def per_device(n, no, pressure, tables, quad_weight, love_number, order_list, cycle_list):
    _, cycles, lon_local = pressure.shape
    local_orders, _, degrees = tables.shape
    bits = n.bit_length() - 1
    share = degrees // n
    groups = len(plan(bits)[0])
    go = local_orders // groups
    uo = local_orders // UNITS
    modes = order_list.shape[0]
    turns = -(-lon_local // LANES)
    fine, cos_q, sin_q, back = [jnp.asarray(table) for table in twiddles(no, lon_local, modes)]
    small = (
        quad_weight[None, :], love_number.reshape(n, share), order_list[None, :], cycle_list[None, :],
        fine, cos_q, sin_q, back,
    )
    hbm = pl.BlockSpec(memory_space=pl.ANY)
    blocks = pltpu.VMEM((groups, n, 2 * go, share), BF16)
    spectrum, field = pl.pallas_call(
        functools.partial(kernel, n, no),
        out_shape=(
            jax.ShapeDtypeStruct((2, local_orders, share), F32),
            jax.ShapeDtypeStruct((2, cycles, lon_local), F32),
        ),
        in_specs=[hbm] * 10,
        out_specs=(hbm, hbm),
        scratch_shapes=[
            pltpu.VMEM((local_orders * cycles, degrees), BF16),
            pltpu.VMEM((2, cycles, lon_local), BF16),
            *[pltpu.VMEM(array.shape, array.dtype) for array in small],
            pltpu.VMEM((no - 1, 2, cycles, lon_local), BF16),
            pltpu.VMEM((no, turns * 2 * cycles, 2 * LANES), BF16),
            pltpu.VMEM((turns * 2 * cycles, 2 * modes), F32),
            pltpu.VMEM((local_orders, 1), jnp.int32),
            pltpu.VMEM((local_orders, modes), BF16),
            pltpu.VMEM((local_orders, 4 * uo * cycles), F32),
            blocks, blocks, blocks,
            pltpu.VMEM((2, local_orders, share), F32),
            pltpu.VMEM((2, cycles, lon_local), F32),
            pltpu.VMEM((4 * cycles, local_orders), F32),
            pltpu.VMEM((turns * 2 * cycles, 2 * modes), BF16),
            pltpu.VMEM((4 * cycles, modes), BF16),
            pltpu.VMEM((no - 1, 4 * cycles, modes), BF16),
            pltpu.SemaphoreType.DMA((UNITS,)),
            pltpu.SemaphoreType.DMA((9,)),
            pltpu.SemaphoreType.DMA((2,)),
            pltpu.SemaphoreType.DMA((2, no - 1)),
            pltpu.SemaphoreType.DMA((2,)),
            pltpu.SemaphoreType.DMA((max(shared_slots(bits, *plan(bits)).values()) + 1,)),
            pltpu.SemaphoreType.DMA((2, no - 1)),
        ],
        compiler_params=pltpu.CompilerParams(
            collective_id=0, has_side_effects=True, vmem_limit_bytes=56 * 1024 * 1024
        ),
    )(pressure, tables.reshape(local_orders * cycles, degrees), *small)
    return pl.pallas_call(
        finish,
        out_shape=(
            jax.ShapeDtypeStruct(spectrum.shape, F32),
            jax.ShapeDtypeStruct(field.shape, F32),
        ),
        in_specs=[hbm, hbm],
        out_specs=(hbm, hbm),
        scratch_shapes=[
            pltpu.VMEM(spectrum.shape, F32),
            pltpu.VMEM(field.shape, F32),
            pltpu.SemaphoreType.DMA((2, 2)),
        ],
    )(spectrum, field)


def solution(mesh):
    placed = (P(None, "lat", "ord"), P("ord", "lat", None), P(), P(), P(), P("lat"))
    return jax.shard_map(
        functools.partial(per_device, mesh.shape["lat"], mesh.shape["ord"]),
        mesh=mesh,
        in_specs=placed,
        out_specs=(P(None, "ord", "lat"), P(None, "lat", "ord")),
        check_vma=False,
    )
```

```python
import functools
import math

import jax
import jax.numpy as jnp
import numpy as np
from jax import lax
from jax.experimental import pallas as pl
from jax.experimental.pallas import tpu as pltpu
from jax.sharding import PartitionSpec as P

DENSITY_RATIO = 3.0 * 1025.0 / 5517.0
LANES = 128
UNITS = 8
STAGGER = 4
MESH = pl.DeviceIdType.MESH
NT = (((1,), (1,)), ((), ()))
F32 = jnp.float32
BF16 = jnp.bfloat16


PLAN_ORDERS = (
    (1, 2, 0, 3), (1, 0, 2, 3), (1, 2, 0, 3), (2, 0, 1, 3), (2, 0, 1, 3), (0, 3, 1, 2),
    (2, 0, 1, 3), (1, 0, 2, 3), (0, 1, 2, 3), (0, 1, 2, 3), (1, 0, 3, 2), (1, 0, 3, 2),
    (1, 0, 2, 3), (0, 3, 1, 2), (2, 3, 1, 0), (2, 0, 1, 3),
)
PLAN_STEPS = (
    96, 192, 32, 64, 97, 113, 160, 224, 193, 128, 98, 209, 0, 81, 114, 49, 177, 33, 99, 225, 161,
    65, 145, 241, 1, 129, 82, 50, 194, 34, 178, 210, 115, 162, 17, 146, 130, 100, 226, 66, 2, 242,
    51, 195, 83, 35, 179, 18, 147, 131, 227, 3, 116, 101, 163, 84, 211, 67, 243, 36, 180, 52, 19,
    196, 228, 148, 132, 4, 117, 212, 164, 85, 102, 68, 181, 244, 37, 53, 20, 197, 149, 5, 133, 118,
    213, 229, 165, 38, 86, 69, 182, 245, 198, 21, 150, 6, 134, 54, 119, 230, 122, 166, 70, 214, 39,
    246, 183, 22, 186, 42, 103, 151, 87, 90, 199, 55, 106, 58, 135, 7, 154, 202, 231, 234, 10, 247,
    167, 120, 71, 215, 218, 121, 250, 23, 40, 138, 41, 26, 184, 104, 152, 185, 105, 74, 153, 200,
    56, 88, 57, 201, 89, 170, 8, 232, 136, 9, 137, 233, 216, 168, 248, 169, 217, 249, 24, 72, 73,
    25,
)


def plan(bits):
    if bits == len(PLAN_ORDERS[0]):
        return [list(order) for order in PLAN_ORDERS], [divmod(code, 16) for code in PLAN_STEPS]
    base = list(range(bits))
    orders = [base]
    if bits >= 3:
        a, b, c, d, e, f = [
            list(head) + base[3:]
            for head in ((0, 1, 2), (1, 0, 2), (2, 0, 1), (2, 1, 0), (0, 2, 1), (1, 2, 0))
        ]
        orders = [a, b, c, e, f, d, a, b]
    orders = [orders[g % len(orders)] for g in range(UNITS)]
    steps = [(g - UNITS, g, 0) for g in range(UNITS)]
    for g in range(UNITS):
        steps += [(g + STAGGER * i, g, i) for i in range(1, 2 * bits + 1)]
        steps.append((g + STAGGER * 2 * bits + 0.5, g, 2 * bits + 1))
        steps.append((g + STAGGER * (2 * bits - 1) + 0.5, g, 2 * bits + 2))
    return orders, [(g, i) for _, g, i in sorted(steps)]


def shared_slots(bits, orders, steps):
    per_unit = len(orders) // UNITS
    take, send = {}, {}
    for at, (g, i) in enumerate(steps):
        if i == 0:
            send.update({(g + v, 0): at for v in range(per_unit)})
        elif i <= 2 * bits:
            take[g, i - 1] = at
            send[g, i] = at

    def along(message):
        g, hop = message
        return orders[g][min(hop, 2 * bits - 1 - hop)]

    free_after, slots = [], {}
    for message in sorted(take, key=lambda m: (send[m], m)):
        known = max(
            (send[m] for m in take if along(m) == along(message) and take[m] <= send[message]),
            default=-1,
        )
        fits = [s for s, at in enumerate(free_after) if at <= known]
        slot = max(fits, key=lambda s: free_after[s]) if fits else len(free_after)
        if not fits:
            free_after.append(0)
        free_after[slot] = take[message]
        slots[message] = slot
    return slots


def permuted(index, order):
    bits = len(order)
    return sum(((index // 2**b) % 2) * 2 ** (bits - 1 - at) for at, b in enumerate(order))


def twiddles(no, lon_local, orders):
    blocks = -(-lon_local // LANES)
    period = no * lon_local

    def turn(positions):
        phase = np.outer(positions, np.arange(orders)) % period
        angle = phase * (2.0 * math.pi / period)
        return np.cos(angle), np.sin(angle)

    fine = np.concatenate(turn(np.arange(LANES)), 1)
    high = fine.astype(BF16)
    low = (fine - high.astype(np.float64)).astype(BF16)
    starts = (lon_local * np.arange(no)[:, None] + LANES * np.arange(blocks)).reshape(-1)
    cos, sin = turn(starts)
    fine = np.concatenate([high, low], 0)
    return fine, cos.astype(np.float32), sin.astype(np.float32), np.ascontiguousarray(fine.T)


def kernel(
    n, no,
    press_hbm, tables_ref, quad_hbm, love_hbm, order_hbm, cycle_hbm, fine_hbm, cos_hbm, sin_hbm, back_hbm,
    spec_hbm, field_hbm,
    tab, press_ref, quad_ref, love_ref, order_ref, cycle_ref, fine, cos_q, sin_q, back,
    gathered, wide, partial, orders_ref, sign_rows, pick, repeated, part, landed, scaled,
    spec_ref, field_ref, signals, rotated, out_signal, in_signal,
    tab_sem, in_sem, spec_sem, press_sem, send_sem, hop_sem, field_sem,
):
    bits = n.bit_length() - 1
    me = lax.axis_index("lat")
    core = lax.axis_index("ord")
    orders_of, steps = plan(bits)
    slots = shared_slots(bits, orders_of, steps)
    groups = len(orders_of)
    per_unit = groups // UNITS
    cycles = press_ref.shape[1]
    lon_local = press_ref.shape[2]
    local_orders = orders_ref.shape[0]
    degrees = tables_ref.shape[1]
    share = degrees // n
    go = local_orders // groups
    rows_g = go * cycles
    uo = local_orders // UNITS
    rows_u = uo * cycles
    both = 2 * cycles
    blocks = max(1, min(n, 1024 // share))
    width = blocks * share
    period = lon_local * no
    turns = cos_q.shape[0] // no
    modes = order_ref.shape[1]

    barrier = pltpu.get_barrier_semaphore()
    partners = []
    for b in range(bits):
        mine = (me // 2**b) % 2
        partners.append(me + (1 - 2 * mine) * 2**b)
    peers = [lax.rem(core + i, no) for i in range(1, no)]
    for peer in peers:
        pl.semaphore_signal(barrier, inc=1, device_id=(me, peer), device_id_type=MESH)
    for partner in partners:
        pl.semaphore_signal(barrier, inc=1, device_id=(partner, core), device_id_type=MESH)

    loads = []
    pairs = (
        (press_hbm, press_ref), (order_hbm, order_ref), (quad_hbm, quad_ref), (cycle_hbm, cycle_ref),
        (fine_hbm, fine), (cos_hbm, cos_q), (sin_hbm, sin_q), (love_hbm, love_ref),
    )
    for i, (source, to) in enumerate(pairs):
        copy = pltpu.make_async_copy(source, to, in_sem.at[i])
        copy.start()
        loads.append(copy)
    loads[0].wait()
    pl.semaphore_wait(barrier, bits + no - 1)
    press_copies = []
    for i, peer in enumerate(peers):
        copy = pltpu.make_async_remote_copy(
            src_ref=press_ref,
            dst_ref=gathered.at[i],
            send_sem=press_sem.at[0, i],
            recv_sem=press_sem.at[1, i],
            device_id=(me, peer),
            device_id_type=MESH,
        )
        copy.start()
        press_copies.append(copy)

    def widen(at, piece):
        for q in range(turns):
            first = q * LANES
            count = min(LANES, lon_local - first)
            rows = jnp.concatenate([piece[h, :, first : first + count].astype(F32) for h in range(2)], 0)
            if count < LANES:
                rows = jnp.concatenate([rows, jnp.zeros((both, LANES - count), F32)], 1)
            rows = rows.astype(BF16)
            wide[at, q * both : (q + 1) * both, :LANES] = rows
            wide[at, q * both : (q + 1) * both, LANES:] = rows

    def transform(at, origin, start):
        partial[...] = jnp.dot(wide[at], fine[...], preferred_element_type=F32)

        cos_sum, sin_sum = start
        for q in range(turns):
            rows = slice(q * both, (q + 1) * both)
            c = partial[rows, :modes]
            s = partial[rows, modes:]
            cq = cos_q[pl.ds(origin * turns + q, 1), :]
            sq = sin_q[pl.ds(origin * turns + q, 1), :]
            cos_sum = cos_sum + (cq * c - sq * s)
            sin_sum = sin_sum + (sq * c + cq * s)
        return cos_sum, sin_sum

    widen(0, press_ref)
    for copy in loads[1:]:
        copy.wait()
    tab_copies = {}
    for u in [g // per_unit for g, i in steps if i == 0]:
        rows = pl.ds(u * rows_u, rows_u)
        copy = pltpu.make_async_copy(tables_ref.at[rows], tab.at[rows], tab_sem.at[u])
        copy.start()
        tab_copies[u] = copy
    back_copy = pltpu.make_async_copy(back_hbm, back, in_sem.at[8])
    back_copy.start()
    shape = (local_orders, modes)
    slot = core * local_orders + lax.broadcasted_iota(jnp.int32, shape, 0)
    lane = lax.broadcasted_iota(jnp.int32, shape, 1)
    order_col = jnp.sum(
        jnp.where(slot == lane, order_ref[...].astype(F32), 0.0), axis=1, keepdims=True
    ).astype(jnp.int32)
    orders_ref[...] = order_col
    pick[...] = jnp.where(order_col == lane, 1.0, 0.0).astype(BF16)

    square = (cycles, cycles)
    eye = lax.broadcasted_iota(jnp.int32, square, 0) == lax.broadcasted_iota(jnp.int32, square, 1)
    cycle_col = jnp.sum(
        jnp.where(eye, cycle_ref[...].astype(F32), 0.0), axis=1, keepdims=True
    ).astype(jnp.int32)
    quad_lane = lax.broadcasted_iota(jnp.int32, (cycles, quad_ref.shape[1]), 1)
    weight = jnp.sum(jnp.where(quad_lane == cycle_col, quad_ref[...], 0.0), axis=1, keepdims=True)
    weight = weight * (1.0 / math.sqrt(quad_ref.shape[1])) * (1.0 / math.sqrt(period))

    col = lax.broadcasted_iota(jnp.int32, (uo, rows_u), 1) // cycles
    row = lax.broadcasted_iota(jnp.int32, (uo, rows_u), 0)
    diagonal = row == col
    spread_row = lax.broadcasted_iota(jnp.int32, (4 * cycles, 4 * rows_u), 0)
    spread_col = lax.broadcasted_iota(jnp.int32, (4 * cycles, 4 * rows_u), 1)
    spread = jnp.where(
        spread_row == (spread_col // rows_u) * cycles + spread_col % cycles, 1.0, 0.0
    ).astype(BF16)
    lane_parity = (order_col + lax.broadcasted_iota(jnp.int32, (local_orders, LANES), 1)) & 1
    sign_rows[...] = jnp.where(lane_parity == 0, 1.0, -1.0)
    lane_order = lax.broadcasted_iota(jnp.int32, (cycles, 4 * go), 1) % go

    zero = jnp.zeros((both, modes), F32)
    sums = transform(0, core, (zero, zero))
    for i, copy in enumerate(press_copies):
        copy.wait()
        widen(i + 1, gathered.at[i])
        sums = transform(i + 1, lax.rem(core + no - 1 - i, no), sums)
    cos_sum, sin_sum = sums
    folded = jnp.concatenate(
        [
            weight * (cos_sum[:cycles] + cos_sum[cycles:]),
            -weight * (sin_sum[:cycles] + sin_sum[cycles:]),
            weight * (cos_sum[:cycles] - cos_sum[cycles:]),
            -weight * (sin_sum[:cycles] - sin_sum[cycles:]),
        ],
        0,
    ).astype(BF16)
    chosen = lax.dot_general(pick[...], folded, NT, preferred_element_type=F32).astype(BF16)
    repeated[...] = jnp.dot(chosen, spread, preferred_element_type=F32)
    def parity(start, count, first):
        degree = first + lax.broadcasted_iota(jnp.int32, (count, width), 1)
        order = orders_ref[start : start + count, :]
        return (degree + order) & 1 == 0, degree >= order

    def region(g, k):
        base = 0
        for at in range(k):
            base = base + ((me // 2 ** orders_of[g][at]) % 2) * (n >> (at + 1))
        return base

    def analyse(u):
        tab_copies[u].wait()
        rows = repeated[u * uo : (u + 1) * uo, :]
        left = jnp.concatenate(
            [jnp.where(diagonal, rows[:, c * rows_u : (c + 1) * rows_u], 0.0) for c in range(4)], 0
        ).astype(BF16)
        for i in range(degrees // width):
            first = i * width
            product = jnp.dot(
                left, tab[u * rows_u : (u + 1) * rows_u, first : first + width],
                preferred_element_type=F32,
            )
            even, present = parity(u * uo, uo, first)
            real = jnp.where(present, jnp.where(even, product[:uo], product[2 * uo : 3 * uo]), 0.0)
            imag = jnp.where(present, jnp.where(even, product[uo : 2 * uo], product[3 * uo :]), 0.0)
            for v in range(per_unit):
                g = u * per_unit + v
                rows = slice(v * go, (v + 1) * go)
                value = jnp.concatenate([real[rows], imag[rows]], 0).astype(BF16)
                for j in range(blocks):
                    to = permuted(i * blocks + j, orders_of[g])
                    part[g, to] = value[:, j * share : (j + 1) * share]

    reduce_copies = {}
    gather_copies = {}

    def send_reduce(g, k):
        h = n >> (k + 1)
        b = orders_of[g][k]
        mine = (me // 2**b) % 2
        copy = pltpu.make_async_remote_copy(
            src_ref=part.at[g, pl.ds(region(g, k) + (1 - mine) * h, h)],
            dst_ref=landed.at[g, pl.ds(n - (n >> k), h)],
            send_sem=send_sem.at[0],
            recv_sem=hop_sem.at[slots[g, k]],
            device_id=(partners[b], core),
            device_id_type=MESH,
        )
        copy.start()
        reduce_copies[g, k] = copy

    def take_reduce(g, k):
        h = n >> (k + 1)
        reduce_copies[g, k].wait_recv()
        keep = region(g, k + 1)
        off = n - (n >> k)
        if k < bits - 1:

            def add(i, carry):
                part[g, keep + i] = (
                    part[g, keep + i].astype(F32) + landed[g, off + i].astype(F32)
                ).astype(BF16)
                return carry

            lax.fori_loop(0, h, add, 0, unroll=min(h, 4))
            send_reduce(g, k + 1)
            return
        total = part[g, keep].astype(F32) + landed[g, off].astype(F32)
        spec_ref[0, g * go : (g + 1) * go, :] = total[:go]
        spec_ref[1, g * go : (g + 1) * go, :] = total[go:]
        scaled[g, keep] = (DENSITY_RATIO * (1.0 + love_ref[pl.ds(me, 1), :]) * total).astype(BF16)
        send_gather(g, bits - 1)

    def send_gather(g, k):
        h = n >> (k + 1)
        b = orders_of[g][k]
        mine = pl.ds(region(g, k + 1), h)
        copy = pltpu.make_async_remote_copy(
            src_ref=scaled.at[g, mine],
            dst_ref=scaled.at[g, mine],
            send_sem=send_sem.at[1],
            recv_sem=hop_sem.at[slots[g, 2 * bits - 1 - k]],
            device_id=(partners[b], core),
            device_id_type=MESH,
        )
        copy.start()
        gather_copies[g, k] = copy

    def take_gather(g, k):
        gather_copies[g, k].wait_recv()
        if k > 0:
            send_gather(g, k - 1)

    def slots_of(g, total):
        piece = jnp.zeros((cycles, 4 * go), F32)
        for o in range(go):
            piece = jnp.where(lane_order == o, total[o * cycles : (o + 1) * cycles], piece)
        return piece

    def keep_signal(g, signal, first):
        signal = signal * (1.0 / math.sqrt(degrees))
        for c in range(4):
            at = slice(c * cycles, (c + 1) * cycles), slice(g * go, (g + 1) * go)
            piece = signal[:, c * go : (c + 1) * go]
            signals[at] = piece if first else signals[at] + piece

    def stacked_of(pieces, signs):
        both_parts = jnp.concatenate(pieces, 1).astype(F32)
        real, imag = both_parts[:go], both_parts[go:]
        return jnp.concatenate([real, imag, real * signs, imag * signs], 0).astype(BF16)

    def synthesise_whole(g):
        signal = jnp.zeros((cycles, 4 * go), F32)
        for i in range(degrees // width):
            first = i * width
            even, _ = parity(g * go, go, first)
            pieces = [scaled[g, permuted(i * blocks + j, orders_of[g])] for j in range(blocks)]
            stacked = stacked_of(pieces, jnp.where(even, 1.0, -1.0))
            total = lax.dot_general(
                tab[g * rows_g : (g + 1) * rows_g, first : first + width], stacked, NT,
                preferred_element_type=F32,
            )
            signal = signal + slots_of(g, total)
        keep_signal(g, signal, True)

    def synthesise_half(g, late):
        order = orders_of[g]
        mine = (me // 2 ** order[0]) % 2
        side = 1 - mine if late else mine
        half = n // 2
        quarter = half // 2
        signs = jnp.concatenate([sign_rows[g * go : (g + 1) * go, :]] * (quarter * share // LANES), 1)
        signal = jnp.zeros((cycles, 4 * go), F32)
        for part_at in range(2):
            pieces, columns = [], []
            for i in range(part_at * quarter, (part_at + 1) * quarter):
                block = side * 2 ** order[0]
                for at in range(1, bits):
                    block = block + ((i >> (bits - 1 - at)) & 1) * 2 ** order[at]
                pieces.append(scaled[g, side * half + i])
                start = pl.multiple_of(block * share, share)
                columns.append(tab[g * rows_g : (g + 1) * rows_g, pl.ds(start, share)])
            total = lax.dot_general(
                jnp.concatenate(columns, 1), stacked_of(pieces, signs), NT, preferred_element_type=F32
            )
            signal = signal + slots_of(g, total)
        keep_signal(g, signal, not late)

    halves = share % LANES == 0 and n >= 4
    spec_copy = pltpu.make_async_copy(spec_ref, spec_hbm, spec_sem.at[0])
    last_sum = max(at for at, (_, i) in enumerate(steps) if i == bits)
    for at, (g, i) in enumerate(steps):
        if at == last_sum + 1:
            spec_copy.start()
        if i == 0:
            analyse(g // per_unit)
            for v in range(per_unit):
                send_reduce(g + v, 0)
        elif i <= bits:
            take_reduce(g, i - 1)
        elif i <= 2 * bits:
            take_gather(g, 2 * bits - i)
        elif not halves:
            if i == 2 * bits + 1:
                synthesise_whole(g)
        else:
            synthesise_half(g, i == 2 * bits + 1)

    back_copy.wait()
    natural = jnp.dot(signals[...].astype(BF16), pick[...], preferred_element_type=F32)
    out_signal[...] = natural.astype(BF16)
    field_copies = []
    for i, peer in enumerate(peers):
        copy = pltpu.make_async_remote_copy(
            src_ref=out_signal,
            dst_ref=in_signal.at[i],
            send_sem=field_sem.at[0, i],
            recv_sem=field_sem.at[1, i],
            device_id=(me, peer),
            device_id_type=MESH,
        )
        copy.start()
        field_copies.append(copy)
    total = natural
    for i, copy in enumerate(field_copies):
        copy.wait_recv()
        total = total + in_signal[i].astype(F32)
    total = total * (1.0 / math.sqrt(modes))
    real = jnp.concatenate([total[:cycles], total[2 * cycles : 3 * cycles]], 0)
    imag = jnp.concatenate([total[cycles : 2 * cycles], total[3 * cycles :]], 0)
    for q in range(turns):
        cq = cos_q[pl.ds(core * turns + q, 1), :]
        sq = sin_q[pl.ds(core * turns + q, 1), :]
        rows = slice(q * both, (q + 1) * both)
        rotated[rows, :modes] = (real * cq - imag * sq).astype(BF16)
        rotated[rows, modes:] = (-real * sq - imag * cq).astype(BF16)
    parts = jnp.dot(rotated[...], back[...], preferred_element_type=F32)
    field = parts[:, :LANES] + parts[:, LANES:]
    for q in range(turns):
        first = q * LANES
        count = min(LANES, lon_local - first)
        for h in range(2):
            at = q * both + h * cycles
            field_ref[h, :, first : first + count] = field[at : at + cycles, :count]
    field_copy = pltpu.make_async_copy(field_ref, field_hbm, spec_sem.at[1])
    field_copy.start()
    for i, blocks_ref in enumerate((part, scaled)):
        sent = blocks_ref.at[:, pl.ds(0, n - 1)]
        pltpu.make_async_copy(sent, sent, send_sem.at[i]).wait()
    for copy in field_copies:
        copy.wait_send()
    spec_copy.wait()
    field_copy.wait()


def finish(half_spec, half_field, spec_ref, field_ref, spec, field, sems):
    pairs = ((half_spec, spec, spec_ref), (half_field, field, field_ref))
    loads = [pltpu.make_async_copy(a, b, sems.at[0, i]) for i, (a, b, _) in enumerate(pairs)]
    stores = [pltpu.make_async_copy(b, c, sems.at[1, i]) for i, (_, b, c) in enumerate(pairs)]
    for load in loads:
        load.start()
    for load, store in zip(loads, stores):
        load.wait()
        store.start()
    for store in stores:
        store.wait()


def per_device(n, no, pressure, tables, quad_weight, love_number, order_list, cycle_list):
    _, cycles, lon_local = pressure.shape
    local_orders, _, degrees = tables.shape
    bits = n.bit_length() - 1
    share = degrees // n
    groups = len(plan(bits)[0])
    go = local_orders // groups
    uo = local_orders // UNITS
    modes = order_list.shape[0]
    turns = -(-lon_local // LANES)
    fine, cos_q, sin_q, back = [jnp.asarray(table) for table in twiddles(no, lon_local, modes)]
    small = (
        quad_weight[None, :], love_number.reshape(n, share), order_list[None, :], cycle_list[None, :],
        fine, cos_q, sin_q, back,
    )
    hbm = pl.BlockSpec(memory_space=pl.ANY)
    blocks = pltpu.VMEM((groups, n, 2 * go, share), BF16)
    spectrum, field = pl.pallas_call(
        functools.partial(kernel, n, no),
        out_shape=(
            jax.ShapeDtypeStruct((2, local_orders, share), F32),
            jax.ShapeDtypeStruct((2, cycles, lon_local), F32),
        ),
        in_specs=[hbm] * 10,
        out_specs=(hbm, hbm),
        scratch_shapes=[
            pltpu.VMEM((local_orders * cycles, degrees), BF16),
            pltpu.VMEM((2, cycles, lon_local), BF16),
            *[pltpu.VMEM(array.shape, array.dtype) for array in small],
            pltpu.VMEM((no - 1, 2, cycles, lon_local), BF16),
            pltpu.VMEM((no, turns * 2 * cycles, 2 * LANES), BF16),
            pltpu.VMEM((turns * 2 * cycles, 2 * modes), F32),
            pltpu.VMEM((local_orders, 1), jnp.int32),
            pltpu.VMEM((local_orders, LANES), F32),
            pltpu.VMEM((local_orders, modes), BF16),
            pltpu.VMEM((local_orders, 4 * uo * cycles), F32),
            blocks, blocks, blocks,
            pltpu.VMEM((2, local_orders, share), F32),
            pltpu.VMEM((2, cycles, lon_local), F32),
            pltpu.VMEM((4 * cycles, local_orders), F32),
            pltpu.VMEM((turns * 2 * cycles, 2 * modes), BF16),
            pltpu.VMEM((4 * cycles, modes), BF16),
            pltpu.VMEM((no - 1, 4 * cycles, modes), BF16),
            pltpu.SemaphoreType.DMA((UNITS,)),
            pltpu.SemaphoreType.DMA((9,)),
            pltpu.SemaphoreType.DMA((2,)),
            pltpu.SemaphoreType.DMA((2, no - 1)),
            pltpu.SemaphoreType.DMA((2,)),
            pltpu.SemaphoreType.DMA((max(shared_slots(bits, *plan(bits)).values()) + 1,)),
            pltpu.SemaphoreType.DMA((2, no - 1)),
        ],
        compiler_params=pltpu.CompilerParams(
            collective_id=0, has_side_effects=True, vmem_limit_bytes=56 * 1024 * 1024
        ),
    )(pressure, tables.reshape(local_orders * cycles, degrees), *small)
    return pl.pallas_call(
        finish,
        out_shape=(
            jax.ShapeDtypeStruct(spectrum.shape, F32),
            jax.ShapeDtypeStruct(field.shape, F32),
        ),
        in_specs=[hbm, hbm],
        out_specs=(hbm, hbm),
        scratch_shapes=[
            pltpu.VMEM(spectrum.shape, F32),
            pltpu.VMEM(field.shape, F32),
            pltpu.SemaphoreType.DMA((2, 2)),
        ],
    )(spectrum, field)


def solution(mesh):
    placed = (P(None, "lat", "ord"), P("ord", "lat", None), P(), P(), P(), P("lat"))
    return jax.shard_map(
        functools.partial(per_device, mesh.shape["lat"], mesh.shape["ord"]),
        mesh=mesh,
        in_specs=placed,
        out_specs=(P(None, "ord", "lat"), P(None, "lat", "ord")),
        check_vma=False,
    )
```

```python
import functools
import math

import jax
import jax.numpy as jnp
import numpy as np
from jax import lax
from jax.experimental import pallas as pl
from jax.experimental.pallas import tpu as pltpu
from jax.sharding import PartitionSpec as P

DENSITY_RATIO = 3.0 * 1025.0 / 5517.0
LANES = 128
UNITS = 8
STAGGER = 4
MESH = pl.DeviceIdType.MESH
NT = (((1,), (1,)), ((), ()))
F32 = jnp.float32
BF16 = jnp.bfloat16


PLAN_ORDERS = (
    (0, 2, 1, 3), (2, 0, 1, 3), (0, 1, 3, 2), (0, 1, 3, 2), (0, 1, 2, 3), (2, 0, 1, 3),
    (2, 0, 1, 3), (1, 3, 0, 2), (1, 2, 0, 3), (2, 0, 3, 1), (1, 0, 2, 3), (1, 0, 2, 3),
    (0, 1, 2, 3), (1, 2, 0, 3), (2, 0, 1, 3), (1, 2, 0, 3),
)
PLAN_STEPS = (
    0, 160, 128, 32, 96, 161, 64, 224, 1, 17, 177, 33, 49, 162, 97, 113, 145, 129, 81, 65, 192, 241,
    178, 98, 34, 225, 163, 2, 146, 50, 114, 18, 66, 82, 242, 179, 209, 193, 130, 99, 3, 35, 226,
    164, 115, 147, 83, 51, 67, 19, 243, 194, 210, 131, 36, 100, 4, 116, 227, 180, 165, 84, 20, 211,
    195, 68, 101, 117, 148, 244, 132, 52, 166, 228, 181, 37, 5, 85, 21, 212, 196, 69, 102, 245, 53,
    149, 133, 182, 6, 229, 38, 118, 22, 213, 197, 70, 246, 167, 86, 134, 230, 170, 54, 183, 150, 39,
    214, 7, 23, 198, 71, 103, 119, 26, 42, 74, 247, 10, 186, 87, 135, 55, 231, 106, 250, 234, 90,
    58, 122, 151, 215, 168, 199, 184, 169, 154, 218, 185, 24, 40, 120, 121, 41, 25, 202, 104, 248,
    8, 249, 105, 9, 138, 136, 72, 88, 89, 137, 56, 232, 233, 73, 57, 216, 200, 152, 153, 201, 217,
)


def plan(bits):
    if bits == len(PLAN_ORDERS[0]):
        return [list(order) for order in PLAN_ORDERS], [divmod(code, 16) for code in PLAN_STEPS]
    base = list(range(bits))
    orders = [base]
    if bits >= 3:
        a, b, c, d, e, f = [
            list(head) + base[3:]
            for head in ((0, 1, 2), (1, 0, 2), (2, 0, 1), (2, 1, 0), (0, 2, 1), (1, 2, 0))
        ]
        orders = [a, b, c, e, f, d, a, b]
    orders = [orders[g % len(orders)] for g in range(UNITS)]
    steps = [(g - UNITS, g, 0) for g in range(UNITS)]
    for g in range(UNITS):
        steps += [(g + STAGGER * i, g, i) for i in range(1, 2 * bits + 1)]
        steps.append((g + STAGGER * 2 * bits + 0.5, g, 2 * bits + 1))
        steps.append((g + STAGGER * (2 * bits - 1) + 0.5, g, 2 * bits + 2))
    return orders, [(g, i) for _, g, i in sorted(steps)]


def shared_slots(bits, orders, steps):
    per_unit = len(orders) // UNITS
    take, send = {}, {}
    for at, (g, i) in enumerate(steps):
        if i == 0:
            send.update({(g + v, 0): at for v in range(per_unit)})
        elif i <= 2 * bits:
            take[g, i - 1] = at
            send[g, i] = at

    def along(message):
        g, hop = message
        return orders[g][min(hop, 2 * bits - 1 - hop)]

    free_after, slots = [], {}
    for message in sorted(take, key=lambda m: (send[m], m)):
        known = max(
            (send[m] for m in take if along(m) == along(message) and take[m] <= send[message]),
            default=-1,
        )
        fits = [s for s, at in enumerate(free_after) if at <= known]
        slot = max(fits, key=lambda s: free_after[s]) if fits else len(free_after)
        if not fits:
            free_after.append(0)
        free_after[slot] = take[message]
        slots[message] = slot
    return slots


def digits(flip, bits, bit):
    if bits < 2:
        return [bit(b) for b in range(bits)]
    first, second = bit(0), bit(1)
    change = flip * (second - first)
    return [first + change, second - change] + [bit(b) for b in range(2, bits)]


def weights(flip, bits):
    if bits < 2:
        return [2**b for b in range(bits)]
    return [1 + flip, 2 - flip] + [2**b for b in range(2, bits)]


def permuted(flip, index, order):
    bits = len(order)
    values = digits(flip, bits, lambda b: (index // 2**b) % 2)
    return sum(values[b] * 2 ** (bits - 1 - at) for at, b in enumerate(order))


def twiddles(no, lon_local, orders):
    blocks = -(-lon_local // LANES)
    period = no * lon_local

    def turn(positions):
        phase = np.outer(positions, np.arange(orders)) % period
        angle = phase * (2.0 * math.pi / period)
        return np.cos(angle), np.sin(angle)

    fine = np.concatenate(turn(np.arange(LANES)), 1)
    high = fine.astype(BF16)
    low = (fine - high.astype(np.float64)).astype(BF16)
    starts = (lon_local * np.arange(no)[:, None] + LANES * np.arange(blocks)).reshape(-1)
    cos, sin = turn(starts)
    fine = np.concatenate([high, low], 0)
    return fine, cos.astype(np.float32), sin.astype(np.float32), np.ascontiguousarray(fine.T)


def kernel(
    n, no,
    press_hbm, tables_ref, quad_hbm, love_hbm, order_hbm, cycle_hbm, fine_hbm, cos_hbm, sin_hbm, back_hbm,
    spec_hbm, field_hbm,
    tab, press_ref, quad_ref, love_ref, order_ref, cycle_ref, fine, cos_q, sin_q, back,
    gathered, wide, partial, orders_ref, sign_rows, pick, repeated, part, landed, scaled,
    spec_ref, field_ref, signals, rotated, out_signal, in_signal,
    tab_sem, in_sem, spec_sem, press_sem, send_sem, hop_sem, field_sem,
):
    bits = n.bit_length() - 1
    me = lax.axis_index("lat")
    core = lax.axis_index("ord")
    orders_of, steps = plan(bits)
    slots = shared_slots(bits, orders_of, steps)
    groups = len(orders_of)
    per_unit = groups // UNITS
    cycles = press_ref.shape[1]
    lon_local = press_ref.shape[2]
    local_orders = orders_ref.shape[0]
    degrees = tables_ref.shape[1]
    share = degrees // n
    go = local_orders // groups
    rows_g = go * cycles
    uo = local_orders // UNITS
    rows_u = uo * cycles
    both = 2 * cycles
    blocks = max(1, min(n, 1024 // share))
    width = blocks * share
    period = lon_local * no
    turns = cos_q.shape[0] // no
    modes = order_ref.shape[1]

    barrier = pltpu.get_barrier_semaphore()
    flip = core % 2
    my_bits = digits(flip, bits, lambda b: (me // 2**b) % 2)
    scale_of = weights(flip, bits)
    partners = [me + (1 - 2 * my_bits[b]) * scale_of[b] for b in range(bits)]
    peers = [lax.rem(core + i, no) for i in range(1, no)]
    for peer in peers:
        pl.semaphore_signal(barrier, inc=1, device_id=(me, peer), device_id_type=MESH)
    for partner in partners:
        pl.semaphore_signal(barrier, inc=1, device_id=(partner, core), device_id_type=MESH)

    loads = []
    pairs = (
        (press_hbm, press_ref), (order_hbm, order_ref), (quad_hbm, quad_ref), (cycle_hbm, cycle_ref),
        (fine_hbm, fine), (cos_hbm, cos_q), (sin_hbm, sin_q), (love_hbm, love_ref),
    )
    for i, (source, to) in enumerate(pairs):
        copy = pltpu.make_async_copy(source, to, in_sem.at[i])
        copy.start()
        loads.append(copy)
    loads[0].wait()
    pl.semaphore_wait(barrier, bits + no - 1)
    press_copies = []
    for i, peer in enumerate(peers):
        copy = pltpu.make_async_remote_copy(
            src_ref=press_ref,
            dst_ref=gathered.at[i],
            send_sem=press_sem.at[0, i],
            recv_sem=press_sem.at[1, i],
            device_id=(me, peer),
            device_id_type=MESH,
        )
        copy.start()
        press_copies.append(copy)

    def widen(at, piece):
        for q in range(turns):
            first = q * LANES
            count = min(LANES, lon_local - first)
            rows = jnp.concatenate([piece[h, :, first : first + count].astype(F32) for h in range(2)], 0)
            if count < LANES:
                rows = jnp.concatenate([rows, jnp.zeros((both, LANES - count), F32)], 1)
            rows = rows.astype(BF16)
            wide[at, q * both : (q + 1) * both, :LANES] = rows
            wide[at, q * both : (q + 1) * both, LANES:] = rows

    def transform(at, origin, start):
        partial[...] = jnp.dot(wide[at], fine[...], preferred_element_type=F32)

        cos_sum, sin_sum = start
        for q in range(turns):
            rows = slice(q * both, (q + 1) * both)
            c = partial[rows, :modes]
            s = partial[rows, modes:]
            cq = cos_q[pl.ds(origin * turns + q, 1), :]
            sq = sin_q[pl.ds(origin * turns + q, 1), :]
            cos_sum = cos_sum + (cq * c - sq * s)
            sin_sum = sin_sum + (sq * c + cq * s)
        return cos_sum, sin_sum

    widen(0, press_ref)
    for copy in loads[1:]:
        copy.wait()
    tab_copies = {}
    for u in [g // per_unit for g, i in steps if i == 0]:
        rows = pl.ds(u * rows_u, rows_u)
        copy = pltpu.make_async_copy(tables_ref.at[rows], tab.at[rows], tab_sem.at[u])
        copy.start()
        tab_copies[u] = copy
    back_copy = pltpu.make_async_copy(back_hbm, back, in_sem.at[8])
    back_copy.start()
    shape = (local_orders, modes)
    slot = core * local_orders + lax.broadcasted_iota(jnp.int32, shape, 0)
    lane = lax.broadcasted_iota(jnp.int32, shape, 1)
    order_col = jnp.sum(
        jnp.where(slot == lane, order_ref[...].astype(F32), 0.0), axis=1, keepdims=True
    ).astype(jnp.int32)
    orders_ref[...] = order_col
    pick[...] = jnp.where(order_col == lane, 1.0, 0.0).astype(BF16)

    square = (cycles, cycles)
    eye = lax.broadcasted_iota(jnp.int32, square, 0) == lax.broadcasted_iota(jnp.int32, square, 1)
    cycle_col = jnp.sum(
        jnp.where(eye, cycle_ref[...].astype(F32), 0.0), axis=1, keepdims=True
    ).astype(jnp.int32)
    quad_lane = lax.broadcasted_iota(jnp.int32, (cycles, quad_ref.shape[1]), 1)
    weight = jnp.sum(jnp.where(quad_lane == cycle_col, quad_ref[...], 0.0), axis=1, keepdims=True)
    weight = weight * (1.0 / math.sqrt(quad_ref.shape[1])) * (1.0 / math.sqrt(period))

    col = lax.broadcasted_iota(jnp.int32, (uo, rows_u), 1) // cycles
    row = lax.broadcasted_iota(jnp.int32, (uo, rows_u), 0)
    diagonal = row == col
    spread_row = lax.broadcasted_iota(jnp.int32, (4 * cycles, 4 * rows_u), 0)
    spread_col = lax.broadcasted_iota(jnp.int32, (4 * cycles, 4 * rows_u), 1)
    spread = jnp.where(
        spread_row == (spread_col // rows_u) * cycles + spread_col % cycles, 1.0, 0.0
    ).astype(BF16)
    lane_parity = (order_col + lax.broadcasted_iota(jnp.int32, (local_orders, LANES), 1)) & 1
    sign_rows[...] = jnp.where(lane_parity == 0, 1.0, -1.0)
    lane_order = lax.broadcasted_iota(jnp.int32, (cycles, 4 * go), 1) % go

    zero = jnp.zeros((both, modes), F32)
    sums = transform(0, core, (zero, zero))
    for i, copy in enumerate(press_copies):
        copy.wait()
        widen(i + 1, gathered.at[i])
        sums = transform(i + 1, lax.rem(core + no - 1 - i, no), sums)
    cos_sum, sin_sum = sums
    folded = jnp.concatenate(
        [
            weight * (cos_sum[:cycles] + cos_sum[cycles:]),
            -weight * (sin_sum[:cycles] + sin_sum[cycles:]),
            weight * (cos_sum[:cycles] - cos_sum[cycles:]),
            -weight * (sin_sum[:cycles] - sin_sum[cycles:]),
        ],
        0,
    ).astype(BF16)
    chosen = lax.dot_general(pick[...], folded, NT, preferred_element_type=F32).astype(BF16)
    repeated[...] = jnp.dot(chosen, spread, preferred_element_type=F32)
    def parity(start, count, first):
        degree = first + lax.broadcasted_iota(jnp.int32, (count, width), 1)
        order = orders_ref[start : start + count, :]
        return (degree + order) & 1 == 0, degree >= order

    def region(g, k):
        base = 0
        for at in range(k):
            base = base + my_bits[orders_of[g][at]] * (n >> (at + 1))
        return base

    def analyse(u):
        tab_copies[u].wait()
        rows = repeated[u * uo : (u + 1) * uo, :]
        left = jnp.concatenate(
            [jnp.where(diagonal, rows[:, c * rows_u : (c + 1) * rows_u], 0.0) for c in range(4)], 0
        ).astype(BF16)
        for i in range(degrees // width):
            first = i * width
            product = jnp.dot(
                left, tab[u * rows_u : (u + 1) * rows_u, first : first + width],
                preferred_element_type=F32,
            )
            even, present = parity(u * uo, uo, first)
            real = jnp.where(present, jnp.where(even, product[:uo], product[2 * uo : 3 * uo]), 0.0)
            imag = jnp.where(present, jnp.where(even, product[uo : 2 * uo], product[3 * uo :]), 0.0)
            for v in range(per_unit):
                g = u * per_unit + v
                rows = slice(v * go, (v + 1) * go)
                value = jnp.concatenate([real[rows], imag[rows]], 0).astype(BF16)
                for j in range(blocks):
                    to = permuted(flip, i * blocks + j, orders_of[g])
                    part[g, to] = value[:, j * share : (j + 1) * share]

    reduce_copies = {}
    gather_copies = {}

    def send_reduce(g, k):
        h = n >> (k + 1)
        b = orders_of[g][k]
        mine = my_bits[b]
        copy = pltpu.make_async_remote_copy(
            src_ref=part.at[g, pl.ds(region(g, k) + (1 - mine) * h, h)],
            dst_ref=landed.at[g, pl.ds(n - (n >> k), h)],
            send_sem=send_sem.at[0],
            recv_sem=hop_sem.at[slots[g, k]],
            device_id=(partners[b], core),
            device_id_type=MESH,
        )
        copy.start()
        reduce_copies[g, k] = copy

    def take_reduce(g, k):
        h = n >> (k + 1)
        reduce_copies[g, k].wait_recv()
        keep = region(g, k + 1)
        off = n - (n >> k)
        if k < bits - 1:

            def add(i, carry):
                part[g, keep + i] = (
                    part[g, keep + i].astype(F32) + landed[g, off + i].astype(F32)
                ).astype(BF16)
                return carry

            lax.fori_loop(0, h, add, 0, unroll=min(h, 4))
            send_reduce(g, k + 1)
            return
        total = part[g, keep].astype(F32) + landed[g, off].astype(F32)
        spec_ref[0, g * go : (g + 1) * go, :] = total[:go]
        spec_ref[1, g * go : (g + 1) * go, :] = total[go:]
        scaled[g, keep] = (DENSITY_RATIO * (1.0 + love_ref[pl.ds(me, 1), :]) * total).astype(BF16)
        send_gather(g, bits - 1)

    def send_gather(g, k):
        h = n >> (k + 1)
        b = orders_of[g][k]
        mine = pl.ds(region(g, k + 1), h)
        copy = pltpu.make_async_remote_copy(
            src_ref=scaled.at[g, mine],
            dst_ref=scaled.at[g, mine],
            send_sem=send_sem.at[1],
            recv_sem=hop_sem.at[slots[g, 2 * bits - 1 - k]],
            device_id=(partners[b], core),
            device_id_type=MESH,
        )
        copy.start()
        gather_copies[g, k] = copy

    def take_gather(g, k):
        gather_copies[g, k].wait_recv()
        if k > 0:
            send_gather(g, k - 1)

    def slots_of(g, total):
        piece = jnp.zeros((cycles, 4 * go), F32)
        for o in range(go):
            piece = jnp.where(lane_order == o, total[o * cycles : (o + 1) * cycles], piece)
        return piece

    def keep_signal(g, signal, first):
        signal = signal * (1.0 / math.sqrt(degrees))
        for c in range(4):
            at = slice(c * cycles, (c + 1) * cycles), slice(g * go, (g + 1) * go)
            piece = signal[:, c * go : (c + 1) * go]
            signals[at] = piece if first else signals[at] + piece

    def stacked_of(pieces, signs):
        both_parts = jnp.concatenate(pieces, 1).astype(F32)
        real, imag = both_parts[:go], both_parts[go:]
        return jnp.concatenate([real, imag, real * signs, imag * signs], 0).astype(BF16)

    def synthesise_whole(g):
        signal = jnp.zeros((cycles, 4 * go), F32)
        for i in range(degrees // width):
            first = i * width
            even, _ = parity(g * go, go, first)
            pieces = [scaled[g, permuted(flip, i * blocks + j, orders_of[g])] for j in range(blocks)]
            stacked = stacked_of(pieces, jnp.where(even, 1.0, -1.0))
            total = lax.dot_general(
                tab[g * rows_g : (g + 1) * rows_g, first : first + width], stacked, NT,
                preferred_element_type=F32,
            )
            signal = signal + slots_of(g, total)
        keep_signal(g, signal, True)

    def synthesise_half(g, late):
        order = orders_of[g]
        mine = my_bits[order[0]]
        side = 1 - mine if late else mine
        half = n // 2
        quarter = half // 2
        signs = jnp.concatenate([sign_rows[g * go : (g + 1) * go, :]] * (quarter * share // LANES), 1)
        signal = jnp.zeros((cycles, 4 * go), F32)
        for part_at in range(2):
            pieces, columns = [], []
            for i in range(part_at * quarter, (part_at + 1) * quarter):
                block = side * scale_of[order[0]]
                for at in range(1, bits):
                    block = block + ((i >> (bits - 1 - at)) & 1) * scale_of[order[at]]
                pieces.append(scaled[g, side * half + i])
                start = pl.multiple_of(block * share, share)
                columns.append(tab[g * rows_g : (g + 1) * rows_g, pl.ds(start, share)])
            total = lax.dot_general(
                jnp.concatenate(columns, 1), stacked_of(pieces, signs), NT, preferred_element_type=F32
            )
            signal = signal + slots_of(g, total)
        keep_signal(g, signal, not late)

    halves = share % LANES == 0 and n >= 4
    spec_copy = pltpu.make_async_copy(spec_ref, spec_hbm, spec_sem.at[0])
    last_sum = max(at for at, (_, i) in enumerate(steps) if i == bits)
    for at, (g, i) in enumerate(steps):
        if at == last_sum + 1:
            spec_copy.start()
        if i == 0:
            analyse(g // per_unit)
            for v in range(per_unit):
                send_reduce(g + v, 0)
        elif i <= bits:
            take_reduce(g, i - 1)
        elif i <= 2 * bits:
            take_gather(g, 2 * bits - i)
        elif not halves:
            if i == 2 * bits + 1:
                synthesise_whole(g)
        else:
            synthesise_half(g, i == 2 * bits + 1)

    back_copy.wait()
    natural = jnp.dot(signals[...].astype(BF16), pick[...], preferred_element_type=F32)
    out_signal[...] = natural.astype(BF16)
    field_copies = []
    for i, peer in enumerate(peers):
        copy = pltpu.make_async_remote_copy(
            src_ref=out_signal,
            dst_ref=in_signal.at[i],
            send_sem=field_sem.at[0, i],
            recv_sem=field_sem.at[1, i],
            device_id=(me, peer),
            device_id_type=MESH,
        )
        copy.start()
        field_copies.append(copy)
    total = natural
    for i, copy in enumerate(field_copies):
        copy.wait_recv()
        total = total + in_signal[i].astype(F32)
    total = total * (1.0 / math.sqrt(modes))
    real = jnp.concatenate([total[:cycles], total[2 * cycles : 3 * cycles]], 0)
    imag = jnp.concatenate([total[cycles : 2 * cycles], total[3 * cycles :]], 0)
    for q in range(turns):
        cq = cos_q[pl.ds(core * turns + q, 1), :]
        sq = sin_q[pl.ds(core * turns + q, 1), :]
        rows = slice(q * both, (q + 1) * both)
        rotated[rows, :modes] = (real * cq - imag * sq).astype(BF16)
        rotated[rows, modes:] = (-real * sq - imag * cq).astype(BF16)
    parts = jnp.dot(rotated[...], back[...], preferred_element_type=F32)
    field = parts[:, :LANES] + parts[:, LANES:]
    for q in range(turns):
        first = q * LANES
        count = min(LANES, lon_local - first)
        for h in range(2):
            at = q * both + h * cycles
            field_ref[h, :, first : first + count] = field[at : at + cycles, :count]
    field_copy = pltpu.make_async_copy(field_ref, field_hbm, spec_sem.at[1])
    field_copy.start()
    for i, blocks_ref in enumerate((part, scaled)):
        sent = blocks_ref.at[:, pl.ds(0, n - 1)]
        pltpu.make_async_copy(sent, sent, send_sem.at[i]).wait()
    for copy in field_copies:
        copy.wait_send()
    spec_copy.wait()
    field_copy.wait()


def finish(half_spec, half_field, spec_ref, field_ref, spec, field, sems):
    pairs = ((half_spec, spec, spec_ref), (half_field, field, field_ref))
    loads = [pltpu.make_async_copy(a, b, sems.at[0, i]) for i, (a, b, _) in enumerate(pairs)]
    stores = [pltpu.make_async_copy(b, c, sems.at[1, i]) for i, (_, b, c) in enumerate(pairs)]
    for load in loads:
        load.start()
    for load, store in zip(loads, stores):
        load.wait()
        store.start()
    for store in stores:
        store.wait()


def per_device(n, no, pressure, tables, quad_weight, love_number, order_list, cycle_list):
    _, cycles, lon_local = pressure.shape
    local_orders, _, degrees = tables.shape
    bits = n.bit_length() - 1
    share = degrees // n
    groups = len(plan(bits)[0])
    go = local_orders // groups
    uo = local_orders // UNITS
    modes = order_list.shape[0]
    turns = -(-lon_local // LANES)
    fine, cos_q, sin_q, back = [jnp.asarray(table) for table in twiddles(no, lon_local, modes)]
    small = (
        quad_weight[None, :], love_number.reshape(n, share), order_list[None, :], cycle_list[None, :],
        fine, cos_q, sin_q, back,
    )
    hbm = pl.BlockSpec(memory_space=pl.ANY)
    blocks = pltpu.VMEM((groups, n, 2 * go, share), BF16)
    spectrum, field = pl.pallas_call(
        functools.partial(kernel, n, no),
        out_shape=(
            jax.ShapeDtypeStruct((2, local_orders, share), F32),
            jax.ShapeDtypeStruct((2, cycles, lon_local), F32),
        ),
        in_specs=[hbm] * 10,
        out_specs=(hbm, hbm),
        scratch_shapes=[
            pltpu.VMEM((local_orders * cycles, degrees), BF16),
            pltpu.VMEM((2, cycles, lon_local), BF16),
            *[pltpu.VMEM(array.shape, array.dtype) for array in small],
            pltpu.VMEM((no - 1, 2, cycles, lon_local), BF16),
            pltpu.VMEM((no, turns * 2 * cycles, 2 * LANES), BF16),
            pltpu.VMEM((turns * 2 * cycles, 2 * modes), F32),
            pltpu.VMEM((local_orders, 1), jnp.int32),
            pltpu.VMEM((local_orders, LANES), F32),
            pltpu.VMEM((local_orders, modes), BF16),
            pltpu.VMEM((local_orders, 4 * uo * cycles), F32),
            blocks, blocks, blocks,
            pltpu.VMEM((2, local_orders, share), F32),
            pltpu.VMEM((2, cycles, lon_local), F32),
            pltpu.VMEM((4 * cycles, local_orders), F32),
            pltpu.VMEM((turns * 2 * cycles, 2 * modes), BF16),
            pltpu.VMEM((4 * cycles, modes), BF16),
            pltpu.VMEM((no - 1, 4 * cycles, modes), BF16),
            pltpu.SemaphoreType.DMA((UNITS,)),
            pltpu.SemaphoreType.DMA((9,)),
            pltpu.SemaphoreType.DMA((2,)),
            pltpu.SemaphoreType.DMA((2, no - 1)),
            pltpu.SemaphoreType.DMA((2,)),
            pltpu.SemaphoreType.DMA((max(shared_slots(bits, *plan(bits)).values()) + 1,)),
            pltpu.SemaphoreType.DMA((2, no - 1)),
        ],
        compiler_params=pltpu.CompilerParams(
            collective_id=0, has_side_effects=True, vmem_limit_bytes=56 * 1024 * 1024
        ),
    )(pressure, tables.reshape(local_orders * cycles, degrees), *small)
    return pl.pallas_call(
        finish,
        out_shape=(
            jax.ShapeDtypeStruct(spectrum.shape, F32),
            jax.ShapeDtypeStruct(field.shape, F32),
        ),
        in_specs=[hbm, hbm],
        out_specs=(hbm, hbm),
        scratch_shapes=[
            pltpu.VMEM(spectrum.shape, F32),
            pltpu.VMEM(field.shape, F32),
            pltpu.SemaphoreType.DMA((2, 2)),
        ],
    )(spectrum, field)


def solution(mesh):
    placed = (P(None, "lat", "ord"), P("ord", "lat", None), P(), P(), P(), P("lat"))
    return jax.shard_map(
        functools.partial(per_device, mesh.shape["lat"], mesh.shape["ord"]),
        mesh=mesh,
        in_specs=placed,
        out_specs=(P(None, "ord", "lat"), P(None, "lat", "ord")),
        check_vma=False,
    )
```

```python
import functools
import math

import jax
import jax.numpy as jnp
import numpy as np
from jax import lax
from jax.experimental import pallas as pl
from jax.experimental.pallas import tpu as pltpu
from jax.sharding import PartitionSpec as P

DENSITY_RATIO = 3.0 * 1025.0 / 5517.0
LANES = 128
UNITS = 8
STAGGER = 4
MESH = pl.DeviceIdType.MESH
NT = (((1,), (1,)), ((), ()))
F32 = jnp.float32
BF16 = jnp.bfloat16


PLAN_ORDERS = (
    (0, 2, 1, 3), (2, 0, 1, 3), (0, 1, 3, 2), (0, 1, 3, 2), (0, 1, 2, 3), (2, 0, 1, 3),
    (2, 0, 1, 3), (1, 3, 0, 2), (1, 2, 0, 3), (2, 0, 3, 1), (1, 0, 2, 3), (1, 0, 2, 3),
    (0, 1, 2, 3), (1, 2, 0, 3), (2, 0, 1, 3), (1, 2, 0, 3),
)
PLAN_STEPS = (
    0, 160, 128, 32, 96, 161, 64, 224, 1, 17, 177, 33, 49, 162, 97, 113, 145, 129, 81, 65, 192, 241,
    178, 98, 34, 225, 163, 2, 146, 50, 114, 18, 66, 82, 242, 179, 209, 193, 130, 99, 3, 35, 226,
    164, 115, 147, 83, 51, 67, 19, 243, 194, 210, 131, 36, 100, 4, 116, 227, 180, 165, 84, 20, 211,
    195, 68, 101, 117, 148, 244, 132, 52, 166, 228, 181, 37, 5, 85, 21, 212, 196, 69, 102, 245, 53,
    149, 133, 182, 6, 229, 38, 118, 22, 213, 197, 70, 246, 167, 86, 134, 230, 170, 54, 183, 150, 39,
    214, 7, 23, 198, 71, 103, 119, 26, 42, 74, 247, 10, 186, 87, 135, 55, 231, 106, 250, 234, 90,
    58, 122, 151, 215, 168, 199, 184, 169, 154, 218, 185, 24, 40, 120, 121, 41, 25, 202, 104, 248,
    8, 249, 105, 9, 138, 136, 72, 88, 89, 137, 56, 232, 233, 73, 57, 216, 200, 152, 153, 201, 217,
)


def plan(bits):
    if bits == len(PLAN_ORDERS[0]):
        return [list(order) for order in PLAN_ORDERS], [divmod(code, 16) for code in PLAN_STEPS]
    base = list(range(bits))
    orders = [base]
    if bits >= 3:
        a, b, c, d, e, f = [
            list(head) + base[3:]
            for head in ((0, 1, 2), (1, 0, 2), (2, 0, 1), (2, 1, 0), (0, 2, 1), (1, 2, 0))
        ]
        orders = [a, b, c, e, f, d, a, b]
    orders = [orders[g % len(orders)] for g in range(UNITS)]
    steps = [(g - UNITS, g, 0) for g in range(UNITS)]
    for g in range(UNITS):
        steps += [(g + STAGGER * i, g, i) for i in range(1, 2 * bits + 1)]
        steps.append((g + STAGGER * 2 * bits + 0.5, g, 2 * bits + 1))
        steps.append((g + STAGGER * (2 * bits - 1) + 0.5, g, 2 * bits + 2))
    return orders, [(g, i) for _, g, i in sorted(steps)]


def shared_slots(bits, orders, steps):
    per_unit = len(orders) // UNITS
    take, send = {}, {}
    for at, (g, i) in enumerate(steps):
        if i == 0:
            send.update({(g + v, 0): at for v in range(per_unit)})
        elif i <= 2 * bits:
            take[g, i - 1] = at
            send[g, i] = at

    def along(message):
        g, hop = message
        return orders[g][min(hop, 2 * bits - 1 - hop)]

    free_after, slots = [], {}
    for message in sorted(take, key=lambda m: (send[m], m)):
        known = max(
            (send[m] for m in take if along(m) == along(message) and take[m] <= send[message]),
            default=-1,
        )
        fits = [s for s, at in enumerate(free_after) if at <= known]
        slot = max(fits, key=lambda s: free_after[s]) if fits else len(free_after)
        if not fits:
            free_after.append(0)
        free_after[slot] = take[message]
        slots[message] = slot
    return slots


def digits(flip, bits, bit):
    if bits < 2:
        return [bit(b) for b in range(bits)]
    first, second = bit(0), bit(1)
    change = flip * (second - first)
    return [first + change, second - change] + [bit(b) for b in range(2, bits)]


def weights(flip, bits):
    if bits < 2:
        return [2**b for b in range(bits)]
    return [1 + flip, 2 - flip] + [2**b for b in range(2, bits)]


def permuted(flip, index, order):
    bits = len(order)
    values = digits(flip, bits, lambda b: (index // 2**b) % 2)
    return sum(values[b] * 2 ** (bits - 1 - at) for at, b in enumerate(order))


def twiddles(no, lon_local, orders):
    blocks = -(-lon_local // LANES)
    period = no * lon_local

    def turn(positions):
        phase = np.outer(positions, np.arange(orders)) % period
        angle = phase * (2.0 * math.pi / period)
        return np.cos(angle), np.sin(angle)

    fine = np.concatenate(turn(np.arange(LANES)), 1)
    high = fine.astype(BF16)
    low = (fine - high.astype(np.float64)).astype(BF16)
    starts = (lon_local * np.arange(no)[:, None] + LANES * np.arange(blocks)).reshape(-1)
    cos, sin = turn(starts)
    fine = np.concatenate([high, low], 0)
    return fine, cos.astype(np.float32), sin.astype(np.float32), np.ascontiguousarray(high.T)


def kernel(
    n, no,
    press_hbm, tables_ref, quad_hbm, love_hbm, order_hbm, cycle_hbm, fine_hbm, cos_hbm, sin_hbm, back_hbm,
    spec_hbm, field_hbm,
    tab, press_ref, quad_ref, love_ref, order_ref, cycle_ref, fine, cos_q, sin_q, back,
    gathered, wide, partial, orders_ref, sign_rows, pick, repeated, part, landed, scaled,
    spec_ref, field_ref, signals, rotated, out_signal, in_signal,
    tab_sem, in_sem, spec_sem, press_sem, send_sem, hop_sem, field_sem,
):
    bits = n.bit_length() - 1
    me = lax.axis_index("lat")
    core = lax.axis_index("ord")
    orders_of, steps = plan(bits)
    slots = shared_slots(bits, orders_of, steps)
    groups = len(orders_of)
    per_unit = groups // UNITS
    cycles = press_ref.shape[1]
    lon_local = press_ref.shape[2]
    local_orders = orders_ref.shape[0]
    degrees = tables_ref.shape[1]
    share = degrees // n
    go = local_orders // groups
    rows_g = go * cycles
    uo = local_orders // UNITS
    rows_u = uo * cycles
    both = 2 * cycles
    blocks = max(1, min(n, 1024 // share))
    width = blocks * share
    period = lon_local * no
    turns = cos_q.shape[0] // no
    modes = order_ref.shape[1]

    barrier = pltpu.get_barrier_semaphore()
    flip = core % 2
    my_bits = digits(flip, bits, lambda b: (me // 2**b) % 2)
    scale_of = weights(flip, bits)
    partners = [me + (1 - 2 * my_bits[b]) * scale_of[b] for b in range(bits)]
    peers = [lax.rem(core + i, no) for i in range(1, no)]
    for peer in peers:
        pl.semaphore_signal(barrier, inc=1, device_id=(me, peer), device_id_type=MESH)
    for partner in partners:
        pl.semaphore_signal(barrier, inc=1, device_id=(partner, core), device_id_type=MESH)

    loads = []
    pairs = (
        (press_hbm, press_ref), (order_hbm, order_ref), (quad_hbm, quad_ref), (cycle_hbm, cycle_ref),
        (fine_hbm, fine), (cos_hbm, cos_q), (sin_hbm, sin_q), (love_hbm, love_ref),
    )
    for i, (source, to) in enumerate(pairs):
        copy = pltpu.make_async_copy(source, to, in_sem.at[i])
        copy.start()
        loads.append(copy)
    loads[0].wait()
    pl.semaphore_wait(barrier, bits + no - 1)
    press_copies = []
    for i, peer in enumerate(peers):
        copy = pltpu.make_async_remote_copy(
            src_ref=press_ref,
            dst_ref=gathered.at[i],
            send_sem=press_sem.at[0, i],
            recv_sem=press_sem.at[1, i],
            device_id=(me, peer),
            device_id_type=MESH,
        )
        copy.start()
        press_copies.append(copy)

    def widen(at, piece):
        for q in range(turns):
            first = q * LANES
            count = min(LANES, lon_local - first)
            rows = jnp.concatenate([piece[h, :, first : first + count].astype(F32) for h in range(2)], 0)
            if count < LANES:
                rows = jnp.concatenate([rows, jnp.zeros((both, LANES - count), F32)], 1)
            rows = rows.astype(BF16)
            wide[at, q * both : (q + 1) * both, :LANES] = rows
            wide[at, q * both : (q + 1) * both, LANES:] = rows

    def transform(at, origin, start):
        partial[...] = jnp.dot(wide[at], fine[...], preferred_element_type=F32)

        cos_sum, sin_sum = start
        for q in range(turns):
            rows = slice(q * both, (q + 1) * both)
            c = partial[rows, :modes]
            s = partial[rows, modes:]
            cq = cos_q[pl.ds(origin * turns + q, 1), :]
            sq = sin_q[pl.ds(origin * turns + q, 1), :]
            cos_sum = cos_sum + (cq * c - sq * s)
            sin_sum = sin_sum + (sq * c + cq * s)
        return cos_sum, sin_sum

    widen(0, press_ref)
    for copy in loads[1:]:
        copy.wait()
    tab_copies = {}
    for u in [g // per_unit for g, i in steps if i == 0]:
        rows = pl.ds(u * rows_u, rows_u)
        copy = pltpu.make_async_copy(tables_ref.at[rows], tab.at[rows], tab_sem.at[u])
        copy.start()
        tab_copies[u] = copy
    back_copy = pltpu.make_async_copy(back_hbm, back, in_sem.at[8])
    back_copy.start()
    shape = (local_orders, modes)
    slot = core * local_orders + lax.broadcasted_iota(jnp.int32, shape, 0)
    lane = lax.broadcasted_iota(jnp.int32, shape, 1)
    order_col = jnp.sum(
        jnp.where(slot == lane, order_ref[...].astype(F32), 0.0), axis=1, keepdims=True
    ).astype(jnp.int32)
    orders_ref[...] = order_col
    pick[...] = jnp.where(order_col == lane, 1.0, 0.0).astype(BF16)

    square = (cycles, cycles)
    eye = lax.broadcasted_iota(jnp.int32, square, 0) == lax.broadcasted_iota(jnp.int32, square, 1)
    cycle_col = jnp.sum(
        jnp.where(eye, cycle_ref[...].astype(F32), 0.0), axis=1, keepdims=True
    ).astype(jnp.int32)
    quad_lane = lax.broadcasted_iota(jnp.int32, (cycles, quad_ref.shape[1]), 1)
    weight = jnp.sum(jnp.where(quad_lane == cycle_col, quad_ref[...], 0.0), axis=1, keepdims=True)
    weight = weight * (1.0 / math.sqrt(quad_ref.shape[1])) * (1.0 / math.sqrt(period))

    col = lax.broadcasted_iota(jnp.int32, (uo, rows_u), 1) // cycles
    row = lax.broadcasted_iota(jnp.int32, (uo, rows_u), 0)
    diagonal = row == col
    spread_row = lax.broadcasted_iota(jnp.int32, (4 * cycles, 4 * rows_u), 0)
    spread_col = lax.broadcasted_iota(jnp.int32, (4 * cycles, 4 * rows_u), 1)
    spread = jnp.where(
        spread_row == (spread_col // rows_u) * cycles + spread_col % cycles, 1.0, 0.0
    ).astype(BF16)
    lane_parity = (order_col + lax.broadcasted_iota(jnp.int32, (local_orders, LANES), 1)) & 1
    sign_rows[...] = jnp.where(lane_parity == 0, 1.0, -1.0)
    lane_order = lax.broadcasted_iota(jnp.int32, (cycles, 4 * go), 1) % go

    zero = jnp.zeros((both, modes), F32)
    sums = transform(0, core, (zero, zero))
    for i, copy in enumerate(press_copies):
        copy.wait()
        widen(i + 1, gathered.at[i])
        sums = transform(i + 1, lax.rem(core + no - 1 - i, no), sums)
    cos_sum, sin_sum = sums
    folded = jnp.concatenate(
        [
            weight * (cos_sum[:cycles] + cos_sum[cycles:]),
            -weight * (sin_sum[:cycles] + sin_sum[cycles:]),
            weight * (cos_sum[:cycles] - cos_sum[cycles:]),
            -weight * (sin_sum[:cycles] - sin_sum[cycles:]),
        ],
        0,
    ).astype(BF16)
    chosen = lax.dot_general(pick[...], folded, NT, preferred_element_type=F32).astype(BF16)
    repeated[...] = jnp.dot(chosen, spread, preferred_element_type=F32)
    def parity(start, count, first):
        degree = first + lax.broadcasted_iota(jnp.int32, (count, width), 1)
        order = orders_ref[start : start + count, :]
        return (degree + order) & 1 == 0, degree >= order

    def region(g, k):
        base = 0
        for at in range(k):
            base = base + my_bits[orders_of[g][at]] * (n >> (at + 1))
        return base

    def analyse(u):
        tab_copies[u].wait()
        rows = repeated[u * uo : (u + 1) * uo, :]
        left = jnp.concatenate(
            [jnp.where(diagonal, rows[:, c * rows_u : (c + 1) * rows_u], 0.0) for c in range(4)], 0
        ).astype(BF16)
        for i in range(degrees // width):
            first = i * width
            product = jnp.dot(
                left, tab[u * rows_u : (u + 1) * rows_u, first : first + width],
                preferred_element_type=F32,
            )
            even, present = parity(u * uo, uo, first)
            real = jnp.where(present, jnp.where(even, product[:uo], product[2 * uo : 3 * uo]), 0.0)
            imag = jnp.where(present, jnp.where(even, product[uo : 2 * uo], product[3 * uo :]), 0.0)
            for v in range(per_unit):
                g = u * per_unit + v
                rows = slice(v * go, (v + 1) * go)
                value = jnp.concatenate([real[rows], imag[rows]], 0).astype(BF16)
                for j in range(blocks):
                    to = permuted(flip, i * blocks + j, orders_of[g])
                    part[g, to] = value[:, j * share : (j + 1) * share]

    reduce_copies = {}
    gather_copies = {}

    def send_reduce(g, k):
        h = n >> (k + 1)
        b = orders_of[g][k]
        mine = my_bits[b]
        copy = pltpu.make_async_remote_copy(
            src_ref=part.at[g, pl.ds(region(g, k) + (1 - mine) * h, h)],
            dst_ref=landed.at[g, pl.ds(n - (n >> k), h)],
            send_sem=send_sem.at[0],
            recv_sem=hop_sem.at[slots[g, k]],
            device_id=(partners[b], core),
            device_id_type=MESH,
        )
        copy.start()
        reduce_copies[g, k] = copy

    def take_reduce(g, k):
        h = n >> (k + 1)
        reduce_copies[g, k].wait_recv()
        keep = region(g, k + 1)
        off = n - (n >> k)
        if k < bits - 1:

            def add(i, carry):
                part[g, keep + i] = (
                    part[g, keep + i].astype(F32) + landed[g, off + i].astype(F32)
                ).astype(BF16)
                return carry

            lax.fori_loop(0, h, add, 0, unroll=min(h, 4))
            send_reduce(g, k + 1)
            return
        total = part[g, keep].astype(F32) + landed[g, off].astype(F32)
        spec_ref[0, g * go : (g + 1) * go, :] = total[:go]
        spec_ref[1, g * go : (g + 1) * go, :] = total[go:]
        scaled[g, keep] = (DENSITY_RATIO * (1.0 + love_ref[pl.ds(me, 1), :]) * total).astype(BF16)
        send_gather(g, bits - 1)

    def send_gather(g, k):
        h = n >> (k + 1)
        b = orders_of[g][k]
        mine = pl.ds(region(g, k + 1), h)
        copy = pltpu.make_async_remote_copy(
            src_ref=scaled.at[g, mine],
            dst_ref=scaled.at[g, mine],
            send_sem=send_sem.at[1],
            recv_sem=hop_sem.at[slots[g, 2 * bits - 1 - k]],
            device_id=(partners[b], core),
            device_id_type=MESH,
        )
        copy.start()
        gather_copies[g, k] = copy

    def take_gather(g, k):
        gather_copies[g, k].wait_recv()
        if k > 0:
            send_gather(g, k - 1)

    def slots_of(g, total):
        piece = jnp.zeros((cycles, 4 * go), F32)
        for o in range(go):
            piece = jnp.where(lane_order == o, total[o * cycles : (o + 1) * cycles], piece)
        return piece

    def keep_signal(g, signal, first):
        signal = signal * (1.0 / math.sqrt(degrees))
        for c in range(4):
            at = slice(c * cycles, (c + 1) * cycles), slice(g * go, (g + 1) * go)
            piece = signal[:, c * go : (c + 1) * go]
            signals[at] = piece if first else signals[at] + piece

    def stacked_of(pieces, signs):
        both_parts = jnp.concatenate(pieces, 1).astype(F32)
        real, imag = both_parts[:go], both_parts[go:]
        return jnp.concatenate([real, imag, real * signs, imag * signs], 0).astype(BF16)

    def synthesise_whole(g):
        signal = jnp.zeros((cycles, 4 * go), F32)
        for i in range(degrees // width):
            first = i * width
            even, _ = parity(g * go, go, first)
            pieces = [scaled[g, permuted(flip, i * blocks + j, orders_of[g])] for j in range(blocks)]
            stacked = stacked_of(pieces, jnp.where(even, 1.0, -1.0))
            total = lax.dot_general(
                tab[g * rows_g : (g + 1) * rows_g, first : first + width], stacked, NT,
                preferred_element_type=F32,
            )
            signal = signal + slots_of(g, total)
        keep_signal(g, signal, True)

    def synthesise_half(g, late):
        order = orders_of[g]
        mine = my_bits[order[0]]
        side = 1 - mine if late else mine
        half = n // 2
        quarter = half // 2
        signs = jnp.concatenate([sign_rows[g * go : (g + 1) * go, :]] * (quarter * share // LANES), 1)
        signal = jnp.zeros((cycles, 4 * go), F32)
        for part_at in range(2):
            pieces, columns = [], []
            for i in range(part_at * quarter, (part_at + 1) * quarter):
                block = side * scale_of[order[0]]
                for at in range(1, bits):
                    block = block + ((i >> (bits - 1 - at)) & 1) * scale_of[order[at]]
                pieces.append(scaled[g, side * half + i])
                start = pl.multiple_of(block * share, share)
                columns.append(tab[g * rows_g : (g + 1) * rows_g, pl.ds(start, share)])
            total = lax.dot_general(
                jnp.concatenate(columns, 1), stacked_of(pieces, signs), NT, preferred_element_type=F32
            )
            signal = signal + slots_of(g, total)
        keep_signal(g, signal, not late)

    halves = share % LANES == 0 and n >= 4
    spec_copy = pltpu.make_async_copy(spec_ref, spec_hbm, spec_sem.at[0])
    last_sum = max(at for at, (_, i) in enumerate(steps) if i == bits)
    for at, (g, i) in enumerate(steps):
        if at == last_sum + 1:
            spec_copy.start()
        if i == 0:
            analyse(g // per_unit)
            for v in range(per_unit):
                send_reduce(g + v, 0)
        elif i <= bits:
            take_reduce(g, i - 1)
        elif i <= 2 * bits:
            take_gather(g, 2 * bits - i)
        elif not halves:
            if i == 2 * bits + 1:
                synthesise_whole(g)
        else:
            synthesise_half(g, i == 2 * bits + 1)

    back_copy.wait()
    natural = jnp.dot(signals[...].astype(BF16), pick[...], preferred_element_type=F32)
    out_signal[...] = natural.astype(BF16)
    field_copies = []
    for i, peer in enumerate(peers):
        copy = pltpu.make_async_remote_copy(
            src_ref=out_signal,
            dst_ref=in_signal.at[i],
            send_sem=field_sem.at[0, i],
            recv_sem=field_sem.at[1, i],
            device_id=(me, peer),
            device_id_type=MESH,
        )
        copy.start()
        field_copies.append(copy)
    total = natural
    for i, copy in enumerate(field_copies):
        copy.wait_recv()
        total = total + in_signal[i].astype(F32)
    total = total * (1.0 / math.sqrt(modes))
    real = jnp.concatenate([total[:cycles], total[2 * cycles : 3 * cycles]], 0)
    imag = jnp.concatenate([total[cycles : 2 * cycles], total[3 * cycles :]], 0)
    for q in range(turns):
        cq = cos_q[pl.ds(core * turns + q, 1), :]
        sq = sin_q[pl.ds(core * turns + q, 1), :]
        rows = slice(q * both, (q + 1) * both)
        rotated[rows, :modes] = (real * cq - imag * sq).astype(BF16)
        rotated[rows, modes:] = (-real * sq - imag * cq).astype(BF16)
    field = jnp.dot(rotated[...], back[...], preferred_element_type=F32)
    for q in range(turns):
        first = q * LANES
        count = min(LANES, lon_local - first)
        for h in range(2):
            at = q * both + h * cycles
            field_ref[h, :, first : first + count] = field[at : at + cycles, :count]
    field_copy = pltpu.make_async_copy(field_ref, field_hbm, spec_sem.at[1])
    field_copy.start()
    for i, blocks_ref in enumerate((part, scaled)):
        sent = blocks_ref.at[:, pl.ds(0, n - 1)]
        pltpu.make_async_copy(sent, sent, send_sem.at[i]).wait()
    for copy in field_copies:
        copy.wait_send()
    spec_copy.wait()
    field_copy.wait()


def finish(half_spec, half_field, spec_ref, field_ref, spec, field, sems):
    pairs = ((half_spec, spec, spec_ref), (half_field, field, field_ref))
    loads = [pltpu.make_async_copy(a, b, sems.at[0, i]) for i, (a, b, _) in enumerate(pairs)]
    stores = [pltpu.make_async_copy(b, c, sems.at[1, i]) for i, (_, b, c) in enumerate(pairs)]
    for load in loads:
        load.start()
    for load, store in zip(loads, stores):
        load.wait()
        store.start()
    for store in stores:
        store.wait()


def per_device(n, no, pressure, tables, quad_weight, love_number, order_list, cycle_list):
    _, cycles, lon_local = pressure.shape
    local_orders, _, degrees = tables.shape
    bits = n.bit_length() - 1
    share = degrees // n
    groups = len(plan(bits)[0])
    go = local_orders // groups
    uo = local_orders // UNITS
    modes = order_list.shape[0]
    turns = -(-lon_local // LANES)
    fine, cos_q, sin_q, back = [jnp.asarray(table) for table in twiddles(no, lon_local, modes)]
    small = (
        quad_weight[None, :], love_number.reshape(n, share), order_list[None, :], cycle_list[None, :],
        fine, cos_q, sin_q, back,
    )
    hbm = pl.BlockSpec(memory_space=pl.ANY)
    blocks = pltpu.VMEM((groups, n, 2 * go, share), BF16)
    spectrum, field = pl.pallas_call(
        functools.partial(kernel, n, no),
        out_shape=(
            jax.ShapeDtypeStruct((2, local_orders, share), F32),
            jax.ShapeDtypeStruct((2, cycles, lon_local), F32),
        ),
        in_specs=[hbm] * 10,
        out_specs=(hbm, hbm),
        scratch_shapes=[
            pltpu.VMEM((local_orders * cycles, degrees), BF16),
            pltpu.VMEM((2, cycles, lon_local), BF16),
            *[pltpu.VMEM(array.shape, array.dtype) for array in small],
            pltpu.VMEM((no - 1, 2, cycles, lon_local), BF16),
            pltpu.VMEM((no, turns * 2 * cycles, 2 * LANES), BF16),
            pltpu.VMEM((turns * 2 * cycles, 2 * modes), F32),
            pltpu.VMEM((local_orders, 1), jnp.int32),
            pltpu.VMEM((local_orders, LANES), F32),
            pltpu.VMEM((local_orders, modes), BF16),
            pltpu.VMEM((local_orders, 4 * uo * cycles), F32),
            blocks, blocks, blocks,
            pltpu.VMEM((2, local_orders, share), F32),
            pltpu.VMEM((2, cycles, lon_local), F32),
            pltpu.VMEM((4 * cycles, local_orders), F32),
            pltpu.VMEM((turns * 2 * cycles, 2 * modes), BF16),
            pltpu.VMEM((4 * cycles, modes), BF16),
            pltpu.VMEM((no - 1, 4 * cycles, modes), BF16),
            pltpu.SemaphoreType.DMA((UNITS,)),
            pltpu.SemaphoreType.DMA((9,)),
            pltpu.SemaphoreType.DMA((2,)),
            pltpu.SemaphoreType.DMA((2, no - 1)),
            pltpu.SemaphoreType.DMA((2,)),
            pltpu.SemaphoreType.DMA((max(shared_slots(bits, *plan(bits)).values()) + 1,)),
            pltpu.SemaphoreType.DMA((2, no - 1)),
        ],
        compiler_params=pltpu.CompilerParams(
            collective_id=0, has_side_effects=True, vmem_limit_bytes=56 * 1024 * 1024
        ),
    )(pressure, tables.reshape(local_orders * cycles, degrees), *small)
    return pl.pallas_call(
        finish,
        out_shape=(
            jax.ShapeDtypeStruct(spectrum.shape, F32),
            jax.ShapeDtypeStruct(field.shape, F32),
        ),
        in_specs=[hbm, hbm],
        out_specs=(hbm, hbm),
        scratch_shapes=[
            pltpu.VMEM(spectrum.shape, F32),
            pltpu.VMEM(field.shape, F32),
            pltpu.SemaphoreType.DMA((2, 2)),
        ],
    )(spectrum, field)


def solution(mesh):
    placed = (P(None, "lat", "ord"), P("ord", "lat", None), P(), P(), P(), P("lat"))
    return jax.shard_map(
        functools.partial(per_device, mesh.shape["lat"], mesh.shape["ord"]),
        mesh=mesh,
        in_specs=placed,
        out_specs=(P(None, "ord", "lat"), P(None, "lat", "ord")),
        check_vma=False,
    )
```
